32 devices in a mesh: section: 4 (over y, core), mp: 8 (over z, x).
Axes of the slice: x: 2, y: 2, z: 4, core: 2. Of those that a mesh axis runs over, the one named last changes fastest.
Arguments:
- arriving: bfloat16 [4, 768, 8192], P('section', None, 'mp'), may hold values from -6 to 6
- norm_gain: bfloat16 [4, 8192], P('section'), may hold values from 0.099609375 to 1.8984375
- w_query: bfloat16 [4, 2048, 8192], P('section', 'mp'), may hold values from -26 to 26
- w_key: bfloat16 [4, 1024, 8192], P('section', 'mp'), may hold values from -1 to 1
- w_value: bfloat16 [4, 1024, 8192], P('section', 'mp'), may hold values from -0.25 to 0.25
- w_out: bfloat16 [4, 2048, 8192], P('section', 'mp'), may hold values from -0.125 to 0.125
Outputs:
- attended: bfloat16 [4, 768, 8192], P('section', 'mp')
- stream_next: bfloat16 [4, 768, 8192], P('section', 'mp')
The draws below stay inside these ranges and needn't reach their ends.
All inputs are finite; a program needn't handle non-finite values.
Results may differ from the reference program's by a relative error of at most 0.017.
Values may be sent and summed in bfloat16 or wider, within the bound.
A program may use at most 128 MiB of HBM per device.

```python
import math
import jax
import jax.numpy as jnp
from jax import lax

D = 8192
HD = 128
KV_HEADS = 8
HQ_DEV = 2
HEADS = 16
KVD = 1024
LENGTH = 768
SECTIONS = 4


def key_rows(key):
    fresh = jax.random.normal(jax.random.fold_in(key, 11), (SECTIONS, KVD, D), jnp.float32)
    return jnp.clip(fresh, -5.0, 5.0) / math.sqrt(D)


def draw_w_key(key, part):
    return key_rows(key).astype(jnp.bfloat16)


def draw_w_query(key, part):
    fresh = jax.random.normal(jax.random.fold_in(key, 23), (SECTIONS, HEADS * HD, D), jnp.float32)
    fresh = jnp.clip(fresh, -5.0, 5.0) / math.sqrt(D)
    return fresh.astype(jnp.bfloat16)


def shard_levels(own_key, shape, cuts, low, largest):
    level = 1.0
    for position, shards_of in cuts:
        draws = jax.random.uniform(jax.random.fold_in(jax.random.fold_in(own_key, 6), position), (shards_of,), jnp.float32, low / len(cuts), largest / len(cuts))
        level = level * jnp.repeat(jnp.exp(draws), shape[position] // shards_of).reshape((-1,) + (1,) * (len(shape) - 1 - position))
    return level


def gaussian(stream_key, shape, scale, most, split=(), held_as=jnp.bfloat16):
    drawn = scale * jax.random.normal(stream_key, shape, jnp.float32)
    if split:
        drawn = drawn * shard_levels(stream_key, shape, split, -0.22, 0.18)
    return jnp.clip(drawn, -most, most).astype(held_as)


def setup_inputs(seed: int = 0) -> dict:
    splits = jax.random.split(jax.random.key(seed), 7)
    return {
        "arriving": gaussian(splits[0], (SECTIONS, LENGTH, D), 1.0, 6.0, ((0, 4), (2, 8))),
        "norm_gain": jnp.clip(1.0 + 0.18 * jax.random.normal(splits[1], (SECTIONS, D), jnp.float32), 0.099609375, 1.8984375).astype(jnp.bfloat16),
        "w_query": draw_w_query(jax.random.fold_in(splits[6], 71), 0),
        "w_key": draw_w_key(jax.random.fold_in(splits[6], 71), 0),
        "w_value": gaussian(splits[4], (SECTIONS, KVD, D), (D // 16) ** -0.5, 0.25, ((0, 4), (1, 8))),
        "w_out": gaussian(splits[5], (SECTIONS, HEADS * HD, D), (HEADS * HD) ** -0.5, 0.125, ((0, 4), (1, 8))),
    }


rope_base = 500000.0
norm_eps = 1e-05

def rotate(channel_major, first_channel):
    channels = channel_major.shape[0]
    length = channel_major.shape[1]
    within = (jnp.arange(channels, dtype=jnp.int32) + first_channel) % HD
    pair_index = (within // 2).astype(channel_major.dtype)
    frequency = jnp.exp(pair_index * (-2.0 * math.log(rope_base) / HD))
    positions = jnp.arange(length, dtype=jnp.int32).astype(channel_major.dtype)
    angles = frequency[0::2, None] * positions[None, :]
    cos_table = jnp.cos(angles)
    sine_table = jnp.sin(angles)
    paired = channel_major.reshape(channels // 2, 2, length)
    even_part = paired[:, 0]
    odd_part = paired[:, 1]
    rotated = jnp.stack([even_part * cos_table - odd_part * sine_table, even_part * sine_table + odd_part * cos_table], axis=1)
    return rotated.reshape(channels, length)

def head_order(pair_major):
    length = pair_major.shape[1]
    grouped = pair_major.reshape(HD // 2, KV_HEADS, 2, length)
    return jnp.transpose(grouped, (1, 0, 2, 3)).reshape(KV_HEADS * HD, length)

def normalize(hidden_in, gain_row):
    as_float = hidden_in.astype(jnp.float32)
    mean_square = lax.optimization_barrier(jnp.mean(as_float * as_float, axis=1, keepdims=True))
    normed = (as_float * lax.rsqrt(mean_square + norm_eps) * gain_row.astype(jnp.float32)).astype(jnp.bfloat16)
    return (as_float, normed)

def reference(arriving, norm_gain, w_query, w_key, w_value, w_out):
    group_size = HEADS // KV_HEADS
    width = HQ_DEV * HD
    score_scale = 1.0 / math.sqrt(HD)
    attended_all = []
    stream_all = []
    for section in range(SECTIONS):
        as_float, normed = normalize(arriving[(section - 1) % SECTIONS], norm_gain[section])
        length = normed.shape[0]
        queries = rotate(jnp.dot(w_query[section], normed.T, preferred_element_type=jnp.float32), 0).astype(jnp.bfloat16)
        key_all = rotate(head_order(jnp.dot(w_key[section], normed.T, preferred_element_type=jnp.float32)), 0).astype(jnp.bfloat16)
        value_all = head_order(jnp.dot(w_value[section], normed.T, preferred_element_type=jnp.float32)).astype(jnp.bfloat16)
        query_heads = queries.reshape(HEADS, HD, length).astype(jnp.float32)
        key_heads = jnp.repeat(key_all.reshape(KV_HEADS, HD, length), group_size, axis=0).astype(jnp.float32)
        value_heads = jnp.repeat(value_all.reshape(KV_HEADS, HD, length), group_size, axis=0).astype(jnp.float32)
        scores = jnp.einsum('hdi,hdj->hij', query_heads, key_heads) * score_scale
        token_index = jnp.arange(length, dtype=jnp.int32)
        causal = token_index[:, None] >= token_index[None, :]
        scores = jnp.where(causal[None], scores, -1e+30)
        row_max = lax.optimization_barrier(jnp.max(scores, axis=-1, keepdims=True))
        exponent = jnp.exp(scores - row_max)
        row_total = lax.optimization_barrier(jnp.sum(exponent, axis=-1, keepdims=True))
        weights = (exponent / row_total).astype(jnp.bfloat16)
        context = jnp.einsum('hij,hdj->ihd', weights.astype(jnp.float32), value_heads).astype(jnp.bfloat16)
        context = context.reshape(length, HEADS * HD)
        summed = jnp.zeros((length, D), jnp.float32)
        for shard in range(HEADS // HQ_DEV):
            partial_term = jnp.dot(context[:, shard * width:(shard + 1) * width], w_out[section][shard * width:(shard + 1) * width], preferred_element_type=jnp.float32)
            summed = summed + lax.optimization_barrier(partial_term.astype(jnp.bfloat16)).astype(jnp.float32)
        attended_all.append(summed.astype(jnp.bfloat16))
        stream_all.append((as_float + summed).astype(jnp.bfloat16))
    return (jnp.stack(attended_all), jnp.stack(stream_all))
```

```python
import functools
import math

import jax
import jax.numpy as jnp
import numpy as np
from jax import lax
from jax.experimental import pallas as pl
from jax.experimental.pallas import tpu as pltpu
from jax.sharding import PartitionSpec as P

HD = 128
KV_HEADS = 8
ROPE_BASE = 500000.0
NORM_EPS = 1e-05
MESH = pl.DeviceIdType.MESH
VMEM_LIMIT = 63500000
EARLY = 9
LATE = 2
LEAD = 4


def ring_position(member, n):
    return jnp.where(member % 2 == 0, member // 2, n - 1 - member // 2)


def ring_member(position, n):
    position = lax.rem(position + 2 * n, n)
    return jnp.where(position < n // 2, 2 * position, 2 * (n - 1 - position) + 1)


def swap_pairs(x):
    lane = lax.broadcasted_iota(jnp.int32, x.shape, 1)
    width = x.shape[1]
    return jnp.where(lane % 2 == 0, pltpu.roll(x, width - 1, 1), pltpu.roll(x, 1, 1))


def ring_kernel(
    n, chunks, pieces, arriving, gain_hbm, wq, wk, wv, w_hbm, tables_hbm,
    attended_ref, stream_ref,
    staged, gain, tables, x_all, weights, acc, squares, sent, got, heads_kv, key_head, value_head, q_ref, w_out, context, running,
    stage_sem, gain_sem, tables_sem, w_sem, wo_sem, shift_send, shift_recv, ring_send, ring_recv, kv_send, kv_recv, send_sem, recv_sem,
):
    sections = lax.axis_size("section")
    section = lax.axis_index("section")
    me = lax.axis_index("mp")
    position = ring_position(me, n)
    right, left = ring_member(position + 1, n), ring_member(position - 1, n)
    following, previous = lax.rem(section + 1, sections), lax.rem(section + sections - 1, sections)
    hops = n // 2
    per = n // chunks
    rows, width = x_all.shape[2:]
    length = n * rows
    chunk_rows = per * rows
    qw, kw, vw = wq.shape[0], wk.shape[0], wv.shape[0]
    heads = qw // HD
    group_size = heads * n // KV_HEADS
    nn = (((1,), (0,)), ((), ()))
    nt = (((1,), (1,)), ((), ()))

    stage = pltpu.make_async_copy(arriving, staged, stage_sem)
    stage.start()
    gain_copy = pltpu.make_async_copy(gain_hbm, gain, gain_sem)
    gain_copy.start()
    tables_copy = pltpu.make_async_copy(tables_hbm, tables, tables_sem)
    tables_copy.start()
    barrier = pltpu.get_barrier_semaphore()
    for step in range(1, n):
        pl.semaphore_signal(barrier, inc=1, device_id={"mp": lax.rem(me + step, n)}, device_id_type=MESH)
    for partner in (following, previous):
        pl.semaphore_signal(barrier, inc=1, device_id={"section": partner}, device_id_type=MESH)

    def weight_copy(j, part):
        src, start, size = ((wq, 0, qw), (wk, qw, kw), (wv, qw + kw, vw))[part]
        return pltpu.make_async_copy(
            src.at[:, pl.ds(j * width, width)], weights.at[j, pl.ds(start, size)], w_sem.at[j, part]
        )

    def shift_copy(c):
        return pltpu.make_async_remote_copy(
            src_ref=staged.at[pl.ds(c * per, per)],
            dst_ref=x_all.at[me, pl.ds(c * per, per)],
            send_sem=shift_send.at[c], recv_sem=shift_recv.at[c],
            device_id={"section": following}, device_id_type=MESH,
        )

    def ring_copy(way, hop, c):
        origin = ring_member(position - (hop - 1) if way == 0 else position + (hop - 1), n)
        return pltpu.make_async_remote_copy(
            src_ref=x_all.at[origin, pl.ds(c * per, per)],
            dst_ref=x_all.at[origin, pl.ds(c * per, per)],
            send_sem=ring_send.at[way, hop - 1, c], recv_sem=ring_recv.at[way, hop - 1, c],
            device_id={"mp": right if way == 0 else left}, device_id_type=MESH,
        )

    for j in range(n):
        for part in range(3):
            weight_copy(j, part).start()
    stage.wait()
    pl.semaphore_wait(barrier, n + 1)
    for c in range(chunks):
        shift_copy(c).start()
    acc[...] = jnp.zeros_like(acc)
    squares[...] = jnp.zeros_like(squares)

    def compute(slot, c):
        x = x_all[slot, pl.ds(c * per, per)].astype(jnp.float32).reshape(chunk_rows, width)
        total = x[:, :128] * x[:, :128]
        for g in range(1, width // 128):
            part = x[:, g * 128 : (g + 1) * 128]
            total = total + part * part
        squares[c] += total
        scaled = (x * gain[slot].astype(jnp.float32)).astype(jnp.bfloat16)
        acc[c] += lax.dot_general(scaled, weights[slot], nt, preferred_element_type=jnp.float32)

    for c in range(chunks):
        shift_copy(c).wait_recv()
        ring_copy(0, 1, c).start()
        ring_copy(1, 1, c).start()
    for j in range(n):
        for part in range(3):
            weight_copy(j, part).wait()
    gain_copy.wait()
    tables_copy.wait()
    wo_copy = pltpu.make_async_copy(w_hbm, w_out, wo_sem)
    wo_copy.start()

    @pl.loop(0, chunks)
    def _(c):
        compute(me, c)

    cos, sin = tables[0], tables[1]
    lane = lax.broadcasted_iota(jnp.int32, (HD, kw), 1)
    source = lax.broadcasted_iota(jnp.int32, (HD, kw), 0)
    pick = (source == (me * kw + lane) // (2 * KV_HEADS) * 2 + lane % 2).astype(jnp.float32)
    k_cos = lax.dot_general(cos, pick, nn, precision=lax.Precision.HIGHEST, preferred_element_type=jnp.float32)
    k_sin = lax.dot_general(sin, pick, nn, precision=lax.Precision.HIGHEST, preferred_element_type=jnp.float32)
    per_head = kw // KV_HEADS
    target = lax.broadcasted_iota(jnp.int32, (kw, kw), 0)
    origin_row = lax.broadcasted_iota(jnp.int32, (kw, kw), 1)
    head, within = target // per_head, target % per_head
    order = (origin_row == (within // 2 * KV_HEADS + head) * 2 + within % 2).astype(jnp.bfloat16)

    @pl.loop(0, hops * chunks)
    def _(i):
        hop = i // chunks + 1
        turn = lax.rem(i, chunks)
        last = hop == hops
        c = jnp.where(last, turn // 2 + lax.rem(turn, 2) * (chunks // 2), turn)
        low = c < chunks // 2
        for way in range(2):
            mine = low if way == 0 else jnp.logical_not(low)

            @pl.when(jnp.logical_or(jnp.logical_not(last), mine))
            def _():
                ring_copy(way, hop, c).wait_recv()

            @pl.when(jnp.logical_and(hop < hops, jnp.logical_or(hop + 1 < hops, mine)))
            def _():
                ring_copy(way, hop + 1, c).start()

        @pl.loop(0, 2)
        def _(way):
            mine = low == (way == 0)

            @pl.when(jnp.logical_or(jnp.logical_not(last), mine))
            def _():
                compute(ring_member(jnp.where(way == 0, position - hop, position + hop), n), c)

    inverse = lax.rsqrt(
        jnp.sum(squares[...].reshape(length, 128), axis=1, keepdims=True) * (1.0 / (n * width)) + NORM_EPS
    )
    k = acc[:, :, qw : qw + kw].reshape(length, kw) * inverse
    k_rot = (k * k_cos + swap_pairs(k) * k_sin).astype(jnp.bfloat16)
    def kv_copy(part, step):
        other = lax.rem(me + step, n)
        return pltpu.make_async_remote_copy(
            src_ref=sent.at[other * heads // group_size, part], dst_ref=got.at[me, part],
            send_sem=kv_send.at[part, step - 1], recv_sem=kv_recv.at[part, step - 1],
            device_id={"mp": other}, device_id_type=MESH,
        )

    def order_and_send(part, channels):
        ordered = lax.dot_general(order, channels, nt, preferred_element_type=jnp.float32)
        for h in range(KV_HEADS):
            sent[h, part] = ordered[h * per_head : (h + 1) * per_head].astype(jnp.bfloat16)
        for step in range(1, n):
            kv_copy(part, step).start()

    order_and_send(0, k_rot)
    order_and_send(1, (acc[:, :, qw + kw :].reshape(length, vw) * inverse).astype(jnp.bfloat16))
    got[me] = sent[me * heads // group_size]
    for h in range(heads):
        q = acc[:, :, h * HD : (h + 1) * HD].reshape(length, HD) * inverse
        q_ref[:, :, h * HD : (h + 1) * HD] = (
            (q * cos + swap_pairs(q) * sin).reshape(n, rows, HD).astype(jnp.bfloat16)
        )

    def receive(part, whole):
        for step in range(1, n):
            kv_copy(part, step).wait_recv()
        for j in range(n):
            heads_kv[part, j * per_head : (j + 1) * per_head] = got[j, part].astype(jnp.float32)
        whole[...] = heads_kv[part].astype(jnp.bfloat16)

    receive(0, key_head)

    piece_width = running.shape[4]
    scale = 1.0 / math.sqrt(HD)

    def attend(block, ready=None):
        row = lax.broadcasted_iota(jnp.int32, (rows, length), 0) + block * rows
        column = lax.broadcasted_iota(jnp.int32, (rows, length), 1)
        probs = []
        for h in range(heads):
            q = q_ref[block, :, h * HD : (h + 1) * HD]
            scores = lax.dot_general(q, key_head[...], nn, preferred_element_type=jnp.float32) * scale
            scores = jnp.where(row >= column, scores, -1e30)
            exponent = jnp.exp(scores - jnp.max(scores, axis=1, keepdims=True))
            probs.append((exponent / jnp.sum(exponent, axis=1, keepdims=True)).astype(jnp.bfloat16))
        if ready is not None:
            ready()
        for h in range(heads):
            context[block, :, h * HD : (h + 1) * HD] = lax.dot_general(
                probs[h], value_head[...], nt, preferred_element_type=jnp.float32
            ).astype(jnp.bfloat16)

    def block_of(way, step):
        return ring_member(position - 1 - step if way == 0 else position + 1 + step, n)

    def term(way, step, piece):
        start = (way * pieces + piece) * piece_width
        return jnp.dot(
            context[block_of(way, step)], w_out[:, start : start + piece_width], preferred_element_type=jnp.float32
        )

    def sum_copy(way, step, piece):
        return pltpu.make_async_remote_copy(
            src_ref=running.at[way, step, piece],
            dst_ref=running.at[way, step + 1, piece],
            send_sem=send_sem.at[way, step, piece], recv_sem=recv_sem.at[way, step, piece],
            device_id={"mp": right if way == 0 else left}, device_id_type=MESH,
        )

    wo_copy.wait()
    for way in range(2):
        attend(block_of(way, 0), functools.partial(receive, 1, value_head) if way == 0 else None)
        for piece in range(pieces):
            running[way, 0, piece] = term(way, 0, piece).astype(jnp.bfloat16)
            sum_copy(way, 0, piece).start()

    def ahead(step):
        @pl.when(step < n // 2)
        def _():
            attend(block_of(0, step))
            attend(block_of(1, step))

        @pl.when(step == n // 2)
        def _():
            attend(me)

    ahead(1)

    @pl.loop(1, n - 1)
    def _(step):
        for piece in range(pieces):
            for way in range(2):
                value = term(way, step, piece)
                sum_copy(way, step - 1, piece).wait_recv()
                running[way, step, piece] = (running[way, step, piece].astype(jnp.float32) + value).astype(jnp.bfloat16)
                sum_copy(way, step, piece).start()
        ahead(step + 1)

    for j in range(n):
        stream_ref[:, j * width : (j + 1) * width] = x_all[j, me]
    for piece in range(pieces):
        for way in range(2):
            value = term(way, n - 1, piece)
            sum_copy(way, n - 2, piece).wait_recv()
            value = running[way, n - 1, piece].astype(jnp.float32) + value
            columns = slice((way * pieces + piece) * piece_width, (way * pieces + piece + 1) * piece_width)
            attended_ref[:, columns] = value.astype(jnp.bfloat16)
            stream_ref[:, columns] = (stream_ref[:, columns].astype(jnp.float32) + value).astype(jnp.bfloat16)

    for c in range(chunks):
        shift_copy(c).wait_send()
    for part in range(2):
        for step in range(1, n):
            kv_copy(part, step).wait_send()

    @pl.loop(0, hops * chunks)
    def _(i):
        hop = i // chunks + 1
        c = lax.rem(i, chunks)
        for way in range(2):
            mine = (c < chunks // 2) if way == 0 else (c >= chunks // 2)

            @pl.when(jnp.logical_or(hop < hops, mine))
            def _():
                ring_copy(way, hop, c).wait_send()

    @pl.loop(0, n - 1)
    def _(step):
        for piece in range(pieces):
            for way in range(2):
                sum_copy(way, step, piece).wait_send()


def grid_kernel(
    n, chunks, pieces, arriving, gain_hbm, wq, wk, wv, w_hbm, tables_hbm,
    attended_ref, stream_ref,
    staged, gain, tables, x_all, weights, acc, squares, sent, got, heads_kv, key_head, value_head, q_ref,
    context, w_half, leaving, entering, summed, final,
    stage_sem, gain_sem, tables_sem, w_sem, shift_send, shift_recv, ring_send, ring_recv, short_send, kv_send, kv_recv,
    wo_own, wo_send, wo_recv, context_send, context_recv, mid_send, mid_recv, final_send, final_recv,
):
    sections = lax.axis_size("section")
    section = lax.axis_index("section")
    me = lax.axis_index("mp")
    position = ring_position(me, n)
    right, left = ring_member(position + 1, n), ring_member(position - 1, n)
    following, previous = lax.rem(section + 1, sections), lax.rem(section + sections - 1, sections)
    hops = n // 2
    per = n // chunks
    rows, width = x_all.shape[2:]
    length = n * rows
    chunk_rows = per * rows
    qw, kw, vw = wq.shape[0], wk.shape[0], wv.shape[0]
    heads = qw // HD
    group_size = heads * n // KV_HEADS
    nn = (((1,), (0,)), ((), ()))
    nt = (((1,), (1,)), ((), ()))

    z, x = me // 2, lax.rem(me, 2)
    half = z // 2
    inner_row = 1 + half
    inner = z == inner_row
    corner = jnp.logical_not(inner)
    out_way = lax.rem(position, 2)
    partner = 2 * z + 1 - x
    opposite = 2 * (2 - half) + x
    beyond = ring_member(jnp.where(out_way == 1, position + 1, position - 1), n)
    slot = jnp.where(inner, 2, 0) + x
    per_half = n // 2
    half_first = half * per_half

    stage = pltpu.make_async_copy(arriving, staged, stage_sem)
    stage.start()
    gain_copy = pltpu.make_async_copy(gain_hbm, gain, gain_sem)
    gain_copy.start()
    tables_copy = pltpu.make_async_copy(tables_hbm, tables, tables_sem)
    tables_copy.start()
    barrier = pltpu.get_barrier_semaphore()
    for step in range(1, n):
        pl.semaphore_signal(barrier, inc=1, device_id={"mp": lax.rem(me + step, n)}, device_id_type=MESH)
    for partner_section in (following, previous):
        pl.semaphore_signal(barrier, inc=1, device_id={"section": partner_section}, device_id_type=MESH)

    def weight_copy(j, part):
        src, start, size = ((wq, 0, qw), (wk, qw, kw), (wv, qw + kw, vw))[part]
        return pltpu.make_async_copy(
            src.at[:, pl.ds(j * width, width)], weights.at[j, pl.ds(start, size)], w_sem.at[j, part]
        )

    def shift_copy(c):
        return pltpu.make_async_remote_copy(
            src_ref=staged.at[pl.ds(c * per, per)],
            dst_ref=x_all.at[me, pl.ds(c * per, per)],
            send_sem=shift_send.at[c], recv_sem=shift_recv.at[c],
            device_id={"section": following}, device_id_type=MESH,
        )

    def ring_copy(way, hop, c):
        origin = ring_member(position - (hop - 1) if way == 0 else position + (hop - 1), n)
        return pltpu.make_async_remote_copy(
            src_ref=x_all.at[origin, pl.ds(c * per, per)],
            dst_ref=x_all.at[origin, pl.ds(c * per, per)],
            send_sem=ring_send.at[way, hop - 1, c], recv_sem=ring_recv.at[way, hop - 1, c],
            device_id={"mp": right if way == 0 else left}, device_id_type=MESH,
        )

    def short_copy(late, c):
        origin = beyond if late else me
        return pltpu.make_async_remote_copy(
            src_ref=x_all.at[origin, pl.ds(c * per, per)],
            dst_ref=x_all.at[origin, pl.ds(c * per, per)],
            send_sem=short_send.at[late, c], recv_sem=ring_recv.at[out_way, hops - 2 + late, c],
            device_id={"mp": partner}, device_id_type=MESH,
        )

    def low_or_high(way, c):
        return c < chunks // 2 if way == 0 else c >= chunks // 2

    def sends(way, hop, c):
        on = jnp.logical_not(jnp.logical_and(jnp.logical_and(corner, out_way == way), hop >= hops - 1))
        return jnp.logical_and(on, jnp.logical_or(hop < hops, low_or_high(way, c)))

    piece_width = w_half.shape[3]

    def wo_source(target, k):
        owner = jnp.where(target == 0, x, 1 - x)
        start = pl.multiple_of(owner * (pieces * piece_width) + k * piece_width, piece_width)
        return w_hbm.at[:, pl.ds(start, piece_width)], 2 * inner_row + owner

    def wo_copy(target, k):
        src, device = wo_source(target, k)
        return pltpu.make_async_remote_copy(
            src_ref=src, dst_ref=w_half.at[k, slot],
            send_sem=wo_send.at[target, k], recv_sem=wo_recv.at[slot, k],
            device_id={"mp": device}, device_id_type=MESH,
        )

    def wo_own_copy(k):
        src, _ = wo_source(0, k)
        return pltpu.make_async_copy(src, w_half.at[k, slot], wo_own.at[k])

    def wo_arrived(s, k):
        return pltpu.make_async_remote_copy(
            src_ref=w_half.at[k, s], dst_ref=w_half.at[k, s],
            send_sem=wo_send.at[0, k], recv_sem=wo_recv.at[s, k],
            device_id={"mp": partner}, device_id_type=MESH,
        )

    for j in range(n):
        for part in range(3):
            weight_copy(j, part).start()
    stage.wait()
    pl.semaphore_wait(barrier, n + 1)
    for c in range(chunks):
        shift_copy(c).start()
    acc[...] = jnp.zeros_like(acc)
    squares[...] = jnp.zeros_like(squares)

    def compute(source, c):
        block = x_all[source, pl.ds(c * per, per)].astype(jnp.float32).reshape(chunk_rows, width)
        total = block[:, :128] * block[:, :128]
        for g in range(1, width // 128):
            part = block[:, g * 128 : (g + 1) * 128]
            total = total + part * part
        squares[c] += total
        scaled = (block * gain[source].astype(jnp.float32)).astype(jnp.bfloat16)
        acc[c] += lax.dot_general(scaled, weights[source], nt, preferred_element_type=jnp.float32)

    for c in range(chunks):
        shift_copy(c).wait_recv()
        ring_copy(0, 1, c).start()
        ring_copy(1, 1, c).start()

        @pl.when(inner)
        def _():
            short_copy(0, c).start()
    for j in range(n):
        for part in range(3):
            weight_copy(j, part).wait()
    gain_copy.wait()
    tables_copy.wait()

    @pl.when(inner)
    def _():
        @pl.loop(0, pieces)
        def _(k):
            wo_own_copy(k).start()

    @pl.loop(0, chunks)
    def _(c):
        compute(me, c)

    cos, sin = tables[0], tables[1]
    lane = lax.broadcasted_iota(jnp.int32, (HD, kw), 1)
    source = lax.broadcasted_iota(jnp.int32, (HD, kw), 0)
    pick = (source == (me * kw + lane) // (2 * KV_HEADS) * 2 + lane % 2).astype(jnp.float32)
    k_cos = lax.dot_general(cos, pick, nn, precision=lax.Precision.HIGHEST, preferred_element_type=jnp.float32)
    k_sin = lax.dot_general(sin, pick, nn, precision=lax.Precision.HIGHEST, preferred_element_type=jnp.float32)
    per_head = kw // KV_HEADS
    target = lax.broadcasted_iota(jnp.int32, (kw, kw), 0)
    origin_row = lax.broadcasted_iota(jnp.int32, (kw, kw), 1)
    head, within = target // per_head, target % per_head
    order = (origin_row == (within // 2 * KV_HEADS + head) * 2 + within % 2).astype(jnp.bfloat16)

    @pl.loop(0, hops * chunks)
    def _(i):
        hop = i // chunks + 1
        turn = lax.rem(i, chunks)
        last = hop == hops
        c = jnp.where(last, turn // 2 + lax.rem(turn, 2) * (chunks // 2), turn)
        low = c < chunks // 2
        for way in range(2):
            mine = low_or_high(way, c)

            @pl.when(jnp.logical_or(jnp.logical_not(last), mine))
            def _():
                ring_copy(way, hop, c).wait_recv()

            @pl.when(jnp.logical_and(hop < hops, sends(way, hop + 1, c)))
            def _():
                ring_copy(way, hop + 1, c).start()

            @pl.when(jnp.logical_and(jnp.logical_and(inner, out_way == way), jnp.logical_and(hop == 1, mine)))
            def _():
                short_copy(1, c).start()

        @pl.when(jnp.logical_and(inner, hop == hops - 2))
        def _():
            wo_copy(1, turn).start()

        early = i - (hops - 3) * chunks

        @pl.when(jnp.logical_and(corner, jnp.logical_and(early >= 0, early < EARLY)))
        def _():
            wo_copy(lax.rem(early, 2), early // 2).start()

        @pl.loop(0, 2)
        def _(way):
            mine = low == (way == 0)

            @pl.when(jnp.logical_or(jnp.logical_not(last), mine))
            def _():
                compute(ring_member(jnp.where(way == 0, position - hop, position + hop), n), c)

    inverse = lax.rsqrt(
        jnp.sum(squares[...].reshape(length, 128), axis=1, keepdims=True) * (1.0 / (n * width)) + NORM_EPS
    )
    k = acc[:, :, qw : qw + kw].reshape(length, kw) * inverse
    k_rot = (k * k_cos + swap_pairs(k) * k_sin).astype(jnp.bfloat16)

    def kv_copy(part, step):
        other = lax.rem(me + step, n)
        return pltpu.make_async_remote_copy(
            src_ref=sent.at[other * heads // group_size, part], dst_ref=got.at[me, part],
            send_sem=kv_send.at[part, step - 1], recv_sem=kv_recv.at[part, step - 1],
            device_id={"mp": other}, device_id_type=MESH,
        )

    def order_and_send(part, channels):
        ordered = lax.dot_general(order, channels, nt, preferred_element_type=jnp.float32)
        for h in range(KV_HEADS):
            sent[h, part] = ordered[h * per_head : (h + 1) * per_head].astype(jnp.bfloat16)
        for step in range(1, n):
            kv_copy(part, step).start()

    order_and_send(0, k_rot)
    order_and_send(1, (acc[:, :, qw + kw :].reshape(length, vw) * inverse).astype(jnp.bfloat16))
    got[me] = sent[me * heads // group_size]
    for h in range(heads):
        q = acc[:, :, h * HD : (h + 1) * HD].reshape(length, HD) * inverse
        q_ref[:, :, h * HD : (h + 1) * HD] = (
            (q * cos + swap_pairs(q) * sin).reshape(n, rows, HD).astype(jnp.bfloat16)
        )

    def receive(part, whole):
        for step in range(1, n):
            kv_copy(part, step).wait_recv()
        for j in range(n):
            heads_kv[part, j * per_head : (j + 1) * per_head] = got[j, part].astype(jnp.float32)
        whole[...] = heads_kv[part].astype(jnp.bfloat16)

    receive(0, key_head)
    receive(1, value_head)

    scale = 1.0 / math.sqrt(HD)

    def attend(block):
        row = lax.broadcasted_iota(jnp.int32, (rows, length), 0) + block * rows
        column = lax.broadcasted_iota(jnp.int32, (rows, length), 1)
        for h in range(heads):
            q = q_ref[block, :, h * HD : (h + 1) * HD]
            scores = lax.dot_general(q, key_head[...], nn, preferred_element_type=jnp.float32) * scale
            scores = jnp.where(row >= column, scores, -1e30)
            exponent = jnp.exp(scores - jnp.max(scores, axis=1, keepdims=True))
            probs = (exponent / jnp.sum(exponent, axis=1, keepdims=True)).astype(jnp.bfloat16)
            context[slot, block, :, h * HD : (h + 1) * HD] = lax.dot_general(
                probs, value_head[...], nt, preferred_element_type=jnp.float32
            ).astype(jnp.bfloat16)

    def context_copy(target, block):
        return pltpu.make_async_remote_copy(
            src_ref=context.at[slot, block], dst_ref=context.at[slot, block],
            send_sem=context_send.at[target, block], recv_sem=context_recv.at[slot, block],
            device_id={"mp": 2 * inner_row + (x if target == 0 else 1 - x)}, device_id_type=MESH,
        )

    def context_arrived(s, block):
        return pltpu.make_async_remote_copy(
            src_ref=context.at[s, block], dst_ref=context.at[s, block],
            send_sem=context_send.at[0, block], recv_sem=context_recv.at[s, block],
            device_id={"mp": partner}, device_id_type=MESH,
        )

    @pl.loop(0, n)
    def _(i):
        block = lax.rem(per_half - half_first + i, n)
        attend(block)

        @pl.when(corner)
        def _():
            context_copy(0, block).start()

        context_copy(1, block).start()

        @pl.when(jnp.logical_and(corner, i >= per_half - 1))
        def _():
            first = EARLY + (i - (per_half - 1)) * LATE

            @pl.loop(first, jnp.minimum(first + LATE, 2 * pieces))
            def _(late):
                wo_copy(lax.rem(late, 2), late // 2).start()

    slots = context.shape[0]

    def term(first, k):
        total = jnp.zeros((per_half * rows, piece_width), jnp.float32)
        for s in range(slots):
            total += jnp.dot(
                context[s, pl.ds(first, per_half)].reshape(per_half * rows, qw), w_half[k, s],
                preferred_element_type=jnp.float32,
            )
        return total

    def mid_copy(k):
        return pltpu.make_async_remote_copy(
            src_ref=leaving.at[k], dst_ref=entering.at[k],
            send_sem=mid_send.at[k], recv_sem=mid_recv.at[k],
            device_id={"mp": opposite}, device_id_type=MESH,
        )

    def final_copy(k, b):
        return pltpu.make_async_remote_copy(
            src_ref=summed.at[k, b], dst_ref=final.at[x, k],
            send_sem=final_send.at[k, b], recv_sem=final_recv.at[x, k],
            device_id={"mp": half_first + b}, device_id_type=MESH,
        )

    def final_arrived(side, k):
        return pltpu.make_async_remote_copy(
            src_ref=final.at[side, k], dst_ref=final.at[side, k],
            send_sem=final_send.at[k, 0], recv_sem=final_recv.at[side, k],
            device_id={"mp": partner}, device_id_type=MESH,
        )

    def contexts_arrived(first):
        for s in range(slots):
            @pl.when(slot != s)
            def _():
                @pl.loop(0, per_half)
                def _(b):
                    context_arrived(s, first + b).wait_recv()

    @pl.when(inner)
    def _():
        contexts_arrived(per_half - half_first)

        @pl.loop(0, pieces + LEAD)
        def _(i):
            @pl.when(i < pieces)
            def _():
                wo_own_copy(i).wait()
                for s in range(slots):
                    @pl.when(slot != s)
                    def _():
                        wo_arrived(s, i).wait_recv()
                leaving[i] = term(per_half - half_first, i).astype(jnp.bfloat16)
                mid_copy(i).start()

            @pl.when(i == LEAD)
            def _():
                contexts_arrived(half_first)

            @pl.when(i >= LEAD)
            def _():
                k = i - LEAD
                value = term(half_first, k)
                mid_copy(k).wait_recv()
                value = value + entering[k].astype(jnp.float32)
                summed[k] = value.astype(jnp.bfloat16).reshape(per_half, rows, piece_width)
                for b in range(per_half):
                    @pl.when(half_first + b != me)
                    def _():
                        final_copy(k, b).start()
                final[x, k] = summed[k, me - half_first]

    @pl.loop(0, pieces)
    def _(k):
        for side in range(2):
            @pl.when(jnp.logical_or(corner, x != side))
            def _():
                final_arrived(side, k).wait_recv()
            start = side * (pieces * piece_width) + k * piece_width
            columns = pl.ds(pl.multiple_of(start, piece_width), piece_width)
            within_block = pl.ds(pl.multiple_of(lax.rem(start, width), piece_width), piece_width)
            value = final[side, k]
            attended_ref[:, columns] = value
            stream_ref[:, columns] = (
                x_all[start // width, me, :, within_block].astype(jnp.float32) + value.astype(jnp.float32)
            ).astype(jnp.bfloat16)

    for c in range(chunks):
        shift_copy(c).wait_send()
    for part in range(2):
        for step in range(1, n):
            kv_copy(part, step).wait_send()

    @pl.loop(0, hops * chunks)
    def _(i):
        hop = i // chunks + 1
        c = lax.rem(i, chunks)
        for way in range(2):
            @pl.when(sends(way, hop, c))
            def _():
                ring_copy(way, hop, c).wait_send()

    @pl.loop(0, n)
    def _(block):
        @pl.when(corner)
        def _():
            context_copy(0, block).wait_send()
        context_copy(1, block).wait_send()

    @pl.loop(0, pieces)
    def _(k):
        wo_copy(1, k).wait_send()

        @pl.when(corner)
        def _():
            wo_copy(0, k).wait_send()

        @pl.when(inner)
        def _():
            mid_copy(k).wait_send()
            for b in range(per_half):
                @pl.when(half_first + b != me)
                def _():
                    final_copy(k, b).wait_send()

    @pl.when(inner)
    def _():
        for c in range(chunks):
            short_copy(0, c).wait_send()

            @pl.when((c < chunks // 2) == (out_way == 0))
            def _():
                short_copy(1, c).wait_send()


def rotary_tables(length):
    pair = (np.arange(HD) // 2).astype(np.float32)
    frequency = np.exp(pair * np.float32(-2.0 * math.log(ROPE_BASE) / HD)).astype(np.float32)
    angles = frequency[None, :] * np.arange(length, dtype=np.float32)[:, None]
    sign = np.where(np.arange(HD) % 2 == 0, -1.0, 1.0).astype(np.float32)
    return np.stack([np.cos(angles), np.sin(angles) * sign]).astype(np.float32)


def local(arriving, norm_gain, w_query, w_key, w_value, w_out):
    n = lax.axis_size("mp")
    length, width = arriving.shape[1:]
    rows = length // n
    full = n * width
    chunks = 8 if n <= 8 else 2
    pieces = 4 if n <= 8 else 2
    qw, kw, vw = w_query.shape[1], w_key.shape[1], w_value.shape[1]
    tables = rotary_tables(length)
    vmem = pl.BlockSpec(memory_space=pltpu.VMEM)
    hbm = pl.BlockSpec(memory_space=pltpu.HBM)
    bf16, f32 = jnp.bfloat16, jnp.float32
    dma = pltpu.SemaphoreType.DMA
    operands = (
        arriving[0].reshape(n, rows, width),
        norm_gain[0].reshape(n, 1, width),
        w_query[0], w_key[0], w_value[0], w_out[0], jnp.asarray(tables),
    )
    shared = [
        pltpu.VMEM((n, rows, width), bf16),
        pltpu.VMEM((n, 1, width), bf16),
        pltpu.VMEM((2, length, HD), f32),
        pltpu.VMEM((n, n, rows, width), bf16),
        pltpu.VMEM((n, qw + kw + vw, width), bf16),
        pltpu.VMEM((chunks, length // chunks, qw + kw + vw), f32),
        pltpu.VMEM((chunks, length // chunks, 128), f32),
        pltpu.VMEM((KV_HEADS, 2, kw // KV_HEADS, length), bf16),
        pltpu.VMEM((n, 2, kw // KV_HEADS, length), bf16),
        pltpu.VMEM((2, HD, length), f32),
        pltpu.VMEM((HD, length), bf16),
        pltpu.VMEM((HD, length), bf16),
        pltpu.VMEM((n, rows, qw), bf16),
    ]
    if n == 8:
        pieces = 8
        piece_width = full // (2 * pieces)
        kernel = grid_kernel
        scratch = shared + [
            pltpu.VMEM((4, n, rows, qw), bf16),
            pltpu.VMEM((pieces, 4, qw, piece_width), bf16),
            pltpu.VMEM((pieces, length // 2, piece_width), bf16),
            pltpu.VMEM((pieces, length // 2, piece_width), bf16),
            pltpu.VMEM((pieces, n // 2, rows, piece_width), bf16),
            pltpu.VMEM((2, pieces, rows, piece_width), bf16),
            dma(()),
            dma(()),
            dma(()),
            dma((n, 3)),
            dma((chunks,)),
            dma((chunks,)),
            dma((2, n // 2, chunks)),
            dma((2, n // 2, chunks)),
            dma((2, chunks)),
            dma((2, n - 1)),
            dma((2, n - 1)),
            dma((pieces,)),
            dma((2, pieces)),
            dma((4, pieces)),
            dma((2, n)),
            dma((4, n)),
            dma((pieces,)),
            dma((pieces,)),
            dma((pieces, n // 2)),
            dma((2, pieces)),
        ]
    else:
        kernel = ring_kernel
        scratch = shared + [
            pltpu.VMEM((qw, full), bf16),
            pltpu.VMEM((n, rows, qw), bf16),
            pltpu.VMEM((2, n, pieces, rows, full // (2 * pieces)), bf16),
            dma(()),
            dma(()),
            dma(()),
            dma((n, 3)),
            dma(()),
            dma((chunks,)),
            dma((chunks,)),
            dma((2, n // 2, chunks)),
            dma((2, n // 2, chunks)),
            dma((2, n - 1)),
            dma((2, n - 1)),
            dma((2, n - 1, pieces)),
            dma((2, n - 1, pieces)),
        ]
    attended, stream = pl.pallas_call(
        functools.partial(kernel, n, chunks, pieces),
        name="layer",
        out_shape=(pltpu.VMEM((rows, full), bf16),) * 2,
        in_specs=[hbm] * 7,
        out_specs=(vmem, vmem),
        scratch_shapes=scratch,
        compiler_params=pltpu.CompilerParams(collective_id=0, has_side_effects=True, vmem_limit_bytes=VMEM_LIMIT),
    )(*operands)
    return (attended[None], stream[None])


def solution(mesh):
    return jax.shard_map(
        local,
        mesh=mesh,
        in_specs=(
            P("section", None, "mp"),
            P("section", None),
            P("section", "mp", None),
            P("section", "mp", None),
            P("section", "mp", None),
            P("section", "mp", None),
        ),
        out_specs=(P("section", "mp", None), P("section", "mp", None)),
        check_vma=False,
    )
```

```python
import functools
import math

import jax
import jax.numpy as jnp
import numpy as np
from jax import lax
from jax.experimental import pallas as pl
from jax.experimental.pallas import tpu as pltpu
from jax.sharding import PartitionSpec as P

HD = 128
KV_HEADS = 8
ROPE_BASE = 500000.0
NORM_EPS = 1e-05
MESH = pl.DeviceIdType.MESH
VMEM_LIMIT = 63500000
AHEAD = 2
LAG = 2
LEAD = 3


def ring_position(member, n):
    return jnp.where(member % 2 == 0, member // 2, n - 1 - member // 2)


def ring_member(position, n):
    position = lax.rem(position + 2 * n, n)
    return jnp.where(position < n // 2, 2 * position, 2 * (n - 1 - position) + 1)


def swap_pairs(x):
    lane = lax.broadcasted_iota(jnp.int32, x.shape, 1)
    width = x.shape[1]
    return jnp.where(lane % 2 == 0, pltpu.roll(x, width - 1, 1), pltpu.roll(x, 1, 1))


def ring_kernel(
    n, chunks, pieces, arriving, gain_hbm, wq, wk, wv, w_hbm, tables_hbm,
    attended_ref, stream_ref,
    staged, gain, tables, x_all, weights, acc, squares, sent, got, heads_kv, key_head, value_head, q_ref, w_out, context, running,
    stage_sem, gain_sem, tables_sem, w_sem, wo_sem, shift_send, shift_recv, ring_send, ring_recv, kv_send, kv_recv, send_sem, recv_sem,
):
    sections = lax.axis_size("section")
    section = lax.axis_index("section")
    me = lax.axis_index("mp")
    position = ring_position(me, n)
    right, left = ring_member(position + 1, n), ring_member(position - 1, n)
    following, previous = lax.rem(section + 1, sections), lax.rem(section + sections - 1, sections)
    hops = n // 2
    per = n // chunks
    rows, width = x_all.shape[2:]
    length = n * rows
    chunk_rows = per * rows
    qw, kw, vw = wq.shape[0], wk.shape[0], wv.shape[0]
    heads = qw // HD
    group_size = heads * n // KV_HEADS
    nn = (((1,), (0,)), ((), ()))
    nt = (((1,), (1,)), ((), ()))

    stage = pltpu.make_async_copy(arriving, staged, stage_sem)
    stage.start()
    gain_copy = pltpu.make_async_copy(gain_hbm, gain, gain_sem)
    gain_copy.start()
    tables_copy = pltpu.make_async_copy(tables_hbm, tables, tables_sem)
    tables_copy.start()
    barrier = pltpu.get_barrier_semaphore()
    for step in range(1, n):
        pl.semaphore_signal(barrier, inc=1, device_id={"mp": lax.rem(me + step, n)}, device_id_type=MESH)
    for partner in (following, previous):
        pl.semaphore_signal(barrier, inc=1, device_id={"section": partner}, device_id_type=MESH)

    def weight_copy(j, part):
        src, start, size = ((wq, 0, qw), (wk, qw, kw), (wv, qw + kw, vw))[part]
        return pltpu.make_async_copy(
            src.at[:, pl.ds(j * width, width)], weights.at[j, pl.ds(start, size)], w_sem.at[j, part]
        )

    def shift_copy(c):
        return pltpu.make_async_remote_copy(
            src_ref=staged.at[pl.ds(c * per, per)],
            dst_ref=x_all.at[me, pl.ds(c * per, per)],
            send_sem=shift_send.at[c], recv_sem=shift_recv.at[c],
            device_id={"section": following}, device_id_type=MESH,
        )

    def ring_copy(way, hop, c):
        origin = ring_member(position - (hop - 1) if way == 0 else position + (hop - 1), n)
        return pltpu.make_async_remote_copy(
            src_ref=x_all.at[origin, pl.ds(c * per, per)],
            dst_ref=x_all.at[origin, pl.ds(c * per, per)],
            send_sem=ring_send.at[way, hop - 1, c], recv_sem=ring_recv.at[way, hop - 1, c],
            device_id={"mp": right if way == 0 else left}, device_id_type=MESH,
        )

    for j in range(n):
        for part in range(3):
            weight_copy(j, part).start()
    stage.wait()
    pl.semaphore_wait(barrier, n + 1)
    for c in range(chunks):
        shift_copy(c).start()
    acc[...] = jnp.zeros_like(acc)
    squares[...] = jnp.zeros_like(squares)

    def compute(slot, c):
        x = x_all[slot, pl.ds(c * per, per)].astype(jnp.float32).reshape(chunk_rows, width)
        total = x[:, :128] * x[:, :128]
        for g in range(1, width // 128):
            part = x[:, g * 128 : (g + 1) * 128]
            total = total + part * part
        squares[c] += total
        scaled = (x * gain[slot].astype(jnp.float32)).astype(jnp.bfloat16)
        acc[c] += lax.dot_general(scaled, weights[slot], nt, preferred_element_type=jnp.float32)

    for c in range(chunks):
        shift_copy(c).wait_recv()
        ring_copy(0, 1, c).start()
        ring_copy(1, 1, c).start()
    for j in range(n):
        for part in range(3):
            weight_copy(j, part).wait()
    gain_copy.wait()
    tables_copy.wait()
    wo_copy = pltpu.make_async_copy(w_hbm, w_out, wo_sem)
    wo_copy.start()

    @pl.loop(0, chunks)
    def _(c):
        compute(me, c)

    cos, sin = tables[0], tables[1]
    lane = lax.broadcasted_iota(jnp.int32, (HD, kw), 1)
    source = lax.broadcasted_iota(jnp.int32, (HD, kw), 0)
    pick = (source == (me * kw + lane) // (2 * KV_HEADS) * 2 + lane % 2).astype(jnp.float32)
    k_cos = lax.dot_general(cos, pick, nn, precision=lax.Precision.HIGHEST, preferred_element_type=jnp.float32)
    k_sin = lax.dot_general(sin, pick, nn, precision=lax.Precision.HIGHEST, preferred_element_type=jnp.float32)
    per_head = kw // KV_HEADS
    target = lax.broadcasted_iota(jnp.int32, (kw, kw), 0)
    origin_row = lax.broadcasted_iota(jnp.int32, (kw, kw), 1)
    head, within = target // per_head, target % per_head
    order = (origin_row == (within // 2 * KV_HEADS + head) * 2 + within % 2).astype(jnp.bfloat16)

    @pl.loop(0, hops * chunks)
    def _(i):
        hop = i // chunks + 1
        turn = lax.rem(i, chunks)
        last = hop == hops
        c = jnp.where(last, turn // 2 + lax.rem(turn, 2) * (chunks // 2), turn)
        low = c < chunks // 2
        for way in range(2):
            mine = low if way == 0 else jnp.logical_not(low)

            @pl.when(jnp.logical_or(jnp.logical_not(last), mine))
            def _():
                ring_copy(way, hop, c).wait_recv()

            @pl.when(jnp.logical_and(hop < hops, jnp.logical_or(hop + 1 < hops, mine)))
            def _():
                ring_copy(way, hop + 1, c).start()

        @pl.loop(0, 2)
        def _(way):
            mine = low == (way == 0)

            @pl.when(jnp.logical_or(jnp.logical_not(last), mine))
            def _():
                compute(ring_member(jnp.where(way == 0, position - hop, position + hop), n), c)

    inverse = lax.rsqrt(
        jnp.sum(squares[...].reshape(length, 128), axis=1, keepdims=True) * (1.0 / (n * width)) + NORM_EPS
    )
    k = acc[:, :, qw : qw + kw].reshape(length, kw) * inverse
    k_rot = (k * k_cos + swap_pairs(k) * k_sin).astype(jnp.bfloat16)
    def kv_copy(part, step):
        other = lax.rem(me + step, n)
        return pltpu.make_async_remote_copy(
            src_ref=sent.at[other * heads // group_size, part], dst_ref=got.at[me, part],
            send_sem=kv_send.at[part, step - 1], recv_sem=kv_recv.at[part, step - 1],
            device_id={"mp": other}, device_id_type=MESH,
        )

    def order_and_send(part, channels):
        ordered = lax.dot_general(order, channels, nt, preferred_element_type=jnp.float32)
        for h in range(KV_HEADS):
            sent[h, part] = ordered[h * per_head : (h + 1) * per_head].astype(jnp.bfloat16)
        for step in range(1, n):
            kv_copy(part, step).start()

    order_and_send(0, k_rot)
    order_and_send(1, (acc[:, :, qw + kw :].reshape(length, vw) * inverse).astype(jnp.bfloat16))
    got[me] = sent[me * heads // group_size]
    for h in range(heads):
        q = acc[:, :, h * HD : (h + 1) * HD].reshape(length, HD) * inverse
        q_ref[:, :, h * HD : (h + 1) * HD] = (
            (q * cos + swap_pairs(q) * sin).reshape(n, rows, HD).astype(jnp.bfloat16)
        )

    def receive(part, whole):
        for step in range(1, n):
            kv_copy(part, step).wait_recv()
        for j in range(n):
            heads_kv[part, j * per_head : (j + 1) * per_head] = got[j, part].astype(jnp.float32)
        whole[...] = heads_kv[part].astype(jnp.bfloat16)

    receive(0, key_head)

    piece_width = running.shape[4]
    scale = 1.0 / math.sqrt(HD)

    def attend(block, ready=None):
        row = lax.broadcasted_iota(jnp.int32, (rows, length), 0) + block * rows
        column = lax.broadcasted_iota(jnp.int32, (rows, length), 1)
        probs = []
        for h in range(heads):
            q = q_ref[block, :, h * HD : (h + 1) * HD]
            scores = lax.dot_general(q, key_head[...], nn, preferred_element_type=jnp.float32) * scale
            scores = jnp.where(row >= column, scores, -1e30)
            exponent = jnp.exp(scores - jnp.max(scores, axis=1, keepdims=True))
            probs.append((exponent / jnp.sum(exponent, axis=1, keepdims=True)).astype(jnp.bfloat16))
        if ready is not None:
            ready()
        for h in range(heads):
            context[block, :, h * HD : (h + 1) * HD] = lax.dot_general(
                probs[h], value_head[...], nt, preferred_element_type=jnp.float32
            ).astype(jnp.bfloat16)

    def block_of(way, step):
        return ring_member(position - 1 - step if way == 0 else position + 1 + step, n)

    def term(way, step, piece):
        start = (way * pieces + piece) * piece_width
        return jnp.dot(
            context[block_of(way, step)], w_out[:, start : start + piece_width], preferred_element_type=jnp.float32
        )

    def sum_copy(way, step, piece):
        return pltpu.make_async_remote_copy(
            src_ref=running.at[way, step, piece],
            dst_ref=running.at[way, step + 1, piece],
            send_sem=send_sem.at[way, step, piece], recv_sem=recv_sem.at[way, step, piece],
            device_id={"mp": right if way == 0 else left}, device_id_type=MESH,
        )

    wo_copy.wait()
    for way in range(2):
        attend(block_of(way, 0), functools.partial(receive, 1, value_head) if way == 0 else None)
        for piece in range(pieces):
            running[way, 0, piece] = term(way, 0, piece).astype(jnp.bfloat16)
            sum_copy(way, 0, piece).start()

    def ahead(step):
        @pl.when(step < n // 2)
        def _():
            attend(block_of(0, step))
            attend(block_of(1, step))

        @pl.when(step == n // 2)
        def _():
            attend(me)

    ahead(1)

    @pl.loop(1, n - 1)
    def _(step):
        for piece in range(pieces):
            for way in range(2):
                value = term(way, step, piece)
                sum_copy(way, step - 1, piece).wait_recv()
                running[way, step, piece] = (running[way, step, piece].astype(jnp.float32) + value).astype(jnp.bfloat16)
                sum_copy(way, step, piece).start()
        ahead(step + 1)

    for j in range(n):
        stream_ref[:, j * width : (j + 1) * width] = x_all[j, me]
    for piece in range(pieces):
        for way in range(2):
            value = term(way, n - 1, piece)
            sum_copy(way, n - 2, piece).wait_recv()
            value = running[way, n - 1, piece].astype(jnp.float32) + value
            columns = slice((way * pieces + piece) * piece_width, (way * pieces + piece + 1) * piece_width)
            attended_ref[:, columns] = value.astype(jnp.bfloat16)
            stream_ref[:, columns] = (stream_ref[:, columns].astype(jnp.float32) + value).astype(jnp.bfloat16)

    for c in range(chunks):
        shift_copy(c).wait_send()
    for part in range(2):
        for step in range(1, n):
            kv_copy(part, step).wait_send()

    @pl.loop(0, hops * chunks)
    def _(i):
        hop = i // chunks + 1
        c = lax.rem(i, chunks)
        for way in range(2):
            mine = (c < chunks // 2) if way == 0 else (c >= chunks // 2)

            @pl.when(jnp.logical_or(hop < hops, mine))
            def _():
                ring_copy(way, hop, c).wait_send()

    @pl.loop(0, n - 1)
    def _(step):
        for piece in range(pieces):
            for way in range(2):
                sum_copy(way, step, piece).wait_send()


def grid_kernel(
    n, chunks, pieces, arriving, gain_hbm, wq, wk, wv, w_hbm, tables_hbm,
    attended_ref, stream_ref,
    staged, gain, tables, x_all, weights, acc, squares, rotary, sent, got, key_head, value_head, q_ref,
    context, w_half, leaving, entering, summed, final,
    stage_sem, gain_sem, tables_sem, w_sem, shift_send, shift_recv, ring_send, ring_recv, short_send, kv_send, kv_recv,
    wo_own, wo_send, wo_recv, context_send, context_recv, mid_send, mid_recv, final_send, final_recv,
):
    sections = lax.axis_size("section")
    section = lax.axis_index("section")
    me = lax.axis_index("mp")
    position = ring_position(me, n)
    right, left = ring_member(position + 1, n), ring_member(position - 1, n)
    following, previous = lax.rem(section + 1, sections), lax.rem(section + sections - 1, sections)
    hops = n // 2
    rows = attended_ref.shape[0]
    length, width = x_all.shape[1:]
    per = length // chunks
    qw, kw, vw = wq.shape[0], wk.shape[0], wv.shape[0]
    heads = qw // HD
    group_size = heads * n // KV_HEADS
    nn = (((1,), (0,)), ((), ()))
    nt = (((1,), (1,)), ((), ()))

    def part_of(c):
        return pl.ds(pl.multiple_of(c * per, per), per)

    z, x = me // 2, lax.rem(me, 2)
    half = z // 2
    inner_row = 1 + half
    inner = z == inner_row
    corner = jnp.logical_not(inner)
    out_way = lax.rem(position, 2)
    partner = 2 * z + 1 - x
    opposite = 2 * (2 - half) + x
    beyond = ring_member(jnp.where(out_way == 1, position + 1, position - 1), n)
    slot = jnp.where(inner, 2, 0) + x
    per_half = n // 2
    half_first = half * per_half

    stage = pltpu.make_async_copy(arriving, staged, stage_sem)
    stage.start()
    gain_copy = pltpu.make_async_copy(gain_hbm, gain, gain_sem)
    gain_copy.start()
    tables_copy = pltpu.make_async_copy(tables_hbm, tables, tables_sem)
    tables_copy.start()
    barrier = pltpu.get_barrier_semaphore()
    for step in range(1, n):
        pl.semaphore_signal(barrier, inc=1, device_id={"mp": lax.rem(me + step, n)}, device_id_type=MESH)
    for partner_section in (following, previous):
        pl.semaphore_signal(barrier, inc=1, device_id={"section": partner_section}, device_id_type=MESH)

    def weight_copy(j, part):
        src, start, size = ((wq, 0, qw), (wk, qw, kw), (wv, qw + kw, vw))[part]
        return pltpu.make_async_copy(
            src.at[:, pl.ds(j * width, width)], weights.at[j, pl.ds(start, size)], w_sem.at[j, part]
        )

    def shift_copy(c):
        return pltpu.make_async_remote_copy(
            src_ref=staged.at[part_of(c)],
            dst_ref=x_all.at[me, part_of(c)],
            send_sem=shift_send.at[c], recv_sem=shift_recv.at[c],
            device_id={"section": following}, device_id_type=MESH,
        )

    def ring_copy(way, hop, c):
        origin = ring_member(position - (hop - 1) if way == 0 else position + (hop - 1), n)
        return pltpu.make_async_remote_copy(
            src_ref=x_all.at[origin, part_of(c)],
            dst_ref=x_all.at[origin, part_of(c)],
            send_sem=ring_send.at[way, hop - 1, c], recv_sem=ring_recv.at[way, hop - 1, c],
            device_id={"mp": right if way == 0 else left}, device_id_type=MESH,
        )

    def short_copy(late, c):
        origin = beyond if late else me
        return pltpu.make_async_remote_copy(
            src_ref=x_all.at[origin, part_of(c)],
            dst_ref=x_all.at[origin, part_of(c)],
            send_sem=short_send.at[late, c], recv_sem=ring_recv.at[out_way, hops - 2 + late, c],
            device_id={"mp": partner}, device_id_type=MESH,
        )

    def own_parity(way, c):
        return lax.rem(c, 2) == way

    def sends(way, hop, c):
        on = jnp.logical_not(jnp.logical_and(jnp.logical_and(corner, out_way == way), hop >= hops - 1))
        return jnp.logical_and(on, jnp.logical_or(hop < hops, own_parity(way, c)))

    piece_width = w_half.shape[3]

    def wo_source(target, k):
        owner = jnp.where(target == 0, x, 1 - x)
        start = pl.multiple_of(owner * (pieces * piece_width) + k * piece_width, piece_width)
        return w_hbm.at[:, pl.ds(start, piece_width)], 2 * inner_row + owner

    def wo_copy(target, k):
        src, device = wo_source(target, k)
        return pltpu.make_async_remote_copy(
            src_ref=src, dst_ref=w_half.at[k, slot],
            send_sem=wo_send.at[target, k], recv_sem=wo_recv.at[slot, k],
            device_id={"mp": device}, device_id_type=MESH,
        )

    def wo_own_copy(k):
        src, _ = wo_source(0, k)
        return pltpu.make_async_copy(src, w_half.at[k, slot], wo_own.at[k])

    def wo_arrived(s, k):
        return pltpu.make_async_remote_copy(
            src_ref=w_half.at[k, s], dst_ref=w_half.at[k, s],
            send_sem=wo_send.at[0, k], recv_sem=wo_recv.at[s, k],
            device_id={"mp": partner}, device_id_type=MESH,
        )

    for j in range(n):
        for part in range(3):
            weight_copy(j, part).start()
    stage.wait()
    pl.semaphore_wait(barrier, n + 1)
    for c in range(chunks):
        shift_copy(c).start()
    acc[...] = jnp.zeros_like(acc)
    squares[...] = jnp.zeros_like(squares)
    key_head[...] = jnp.zeros_like(key_head)
    value_head[...] = jnp.zeros_like(value_head)

    def compute(source, c):
        block = x_all[source, part_of(c)].astype(jnp.float32)
        total = block[:, :128] * block[:, :128]
        for g in range(1, width // 128):
            part = block[:, g * 128 : (g + 1) * 128]
            total = total + part * part
        squares[c] += total
        scaled = (block * gain[source].astype(jnp.float32)).astype(jnp.bfloat16)
        acc[c] += lax.dot_general(scaled, weights[source], nt, preferred_element_type=jnp.float32)

    def start_own(c):
        shift_copy(c).wait_recv()
        ring_copy(0, 1, c).start()
        ring_copy(1, 1, c).start()

        @pl.when(inner)
        def _():
            short_copy(0, c).start()

    for c in range(AHEAD):
        start_own(c)
    for j in range(n):
        for part in range(3):
            weight_copy(j, part).wait()
    gain_copy.wait()
    tables_copy.wait()

    @pl.when(inner)
    def _():
        @pl.loop(0, pieces)
        def _(k):
            wo_own_copy(k).start()

    lane = lax.broadcasted_iota(jnp.int32, (HD, kw), 1)
    source = lax.broadcasted_iota(jnp.int32, (HD, kw), 0)
    pick = (source == (me * kw + lane) // (2 * KV_HEADS) * 2 + lane % 2).astype(jnp.float32)
    for t in range(2):
        picked = lax.dot_general(
            tables[t].reshape(length, HD), pick, nn, precision=lax.Precision.HIGHEST, preferred_element_type=jnp.float32
        )
        rotary[t] = picked.reshape(chunks, per, kw)
    per_head = kw // KV_HEADS
    target = lax.broadcasted_iota(jnp.int32, (kw, kw), 0)
    origin_row = lax.broadcasted_iota(jnp.int32, (kw, kw), 1)
    head, within = target // per_head, target % per_head
    order = (origin_row == (within // 2 * KV_HEADS + head) * 2 + within % 2).astype(jnp.bfloat16)

    def kv_copy(c, step):
        other = lax.rem(me + step, n)
        return pltpu.make_async_remote_copy(
            src_ref=sent.at[c, other * heads // group_size], dst_ref=got.at[c, me],
            send_sem=kv_send.at[c, step - 1], recv_sem=kv_recv.at[c, step - 1],
            device_id={"mp": other}, device_id_type=MESH,
        )

    def project(c):
        inverse = lax.rsqrt(jnp.sum(squares[c], axis=1, keepdims=True) * (1.0 / (n * width)) + NORM_EPS)
        k = acc[c, :, qw : qw + kw] * inverse
        k_rot = (k * rotary[0, c] + swap_pairs(k) * rotary[1, c]).astype(jnp.bfloat16)
        v = (acc[c, :, qw + kw :] * inverse).astype(jnp.bfloat16)
        for part, channels in enumerate((k_rot, v)):
            ordered = lax.dot_general(order, channels, nt, preferred_element_type=jnp.float32)
            for h in range(KV_HEADS):
                sent[c, h, part] = ordered[h * per_head : (h + 1) * per_head].astype(jnp.bfloat16)
        for step in range(1, n):
            kv_copy(c, step).start()
        got[c, me] = sent[c, me * heads // group_size]
        for h in range(heads):
            q = acc[c, :, h * HD : (h + 1) * HD] * inverse
            q_ref[c, :, h * HD : (h + 1) * HD] = (q * tables[0, c] + swap_pairs(q) * tables[1, c]).astype(jnp.bfloat16)

    scale = 1.0 / math.sqrt(HD)

    def attend(c):
        for step in range(1, n):
            kv_copy(c, step).wait_recv()
        for j in range(n):
            key_head[j * per_head : (j + 1) * per_head, part_of(c)] = got[c, j, 0]
            value_head[j * per_head : (j + 1) * per_head, part_of(c)] = got[c, j, 1]
        row = lax.broadcasted_iota(jnp.int32, (per, length), 0) + c * per
        column = lax.broadcasted_iota(jnp.int32, (per, length), 1)
        for h in range(heads):
            q = q_ref[c, :, h * HD : (h + 1) * HD]
            scores = lax.dot_general(q, key_head[...], nn, preferred_element_type=jnp.float32) * scale
            scores = jnp.where(row >= column, scores, -1e30)
            exponent = jnp.exp(scores - jnp.max(scores, axis=1, keepdims=True))
            probs = (exponent / jnp.sum(exponent, axis=1, keepdims=True)).astype(jnp.bfloat16)
            context[slot, part_of(c), h * HD : (h + 1) * HD] = lax.dot_general(
                probs, value_head[...], nt, preferred_element_type=jnp.float32
            ).astype(jnp.bfloat16)

        @pl.when(corner)
        def _():
            context_copy(0, c).start()

        context_copy(1, c).start()

    def context_copy(target, c):
        return pltpu.make_async_remote_copy(
            src_ref=context.at[slot, part_of(c)], dst_ref=context.at[slot, part_of(c)],
            send_sem=context_send.at[target, c], recv_sem=context_recv.at[slot, c],
            device_id={"mp": 2 * inner_row + (x if target == 0 else 1 - x)}, device_id_type=MESH,
        )

    def context_arrived(s, c):
        return pltpu.make_async_remote_copy(
            src_ref=context.at[s, part_of(c)], dst_ref=context.at[s, part_of(c)],
            send_sem=context_send.at[0, c], recv_sem=context_recv.at[s, c],
            device_id={"mp": partner}, device_id_type=MESH,
        )

    early_pieces = chunks + chunks // 2

    def wo_range(first, last):
        @pl.loop(first, last)
        def _(i):
            wo_copy(lax.rem(i, 2), i // 2).start()

    @pl.loop(0, chunks + hops - 1)
    def _(wave):
        @pl.when(wave + AHEAD < chunks)
        def _():
            start_own(wave + AHEAD)

        @pl.when(wave < chunks)
        def _():
            compute(me, wave)

        @pl.loop(1, hops + 1)
        def _(hop):
            c = wave - (hop - 1)
            last = hop == hops

            @pl.when(jnp.logical_and(c >= 0, c < chunks))
            def _():
                for way in range(2):
                    mine = own_parity(way, c)

                    @pl.when(jnp.logical_or(jnp.logical_not(last), mine))
                    def _():
                        ring_copy(way, hop, c).wait_recv()

                    @pl.when(jnp.logical_and(hop < hops, sends(way, hop + 1, c)))
                    def _():
                        ring_copy(way, hop + 1, c).start()

                    @pl.when(jnp.logical_and(jnp.logical_and(inner, out_way == way), jnp.logical_and(hop == 1, mine)))
                    def _():
                        short_copy(1, c).start()

                @pl.when(jnp.logical_and(inner, hop == hops - 2))
                def _():
                    @pl.loop(c * pieces // chunks, (c + 1) * pieces // chunks)
                    def _(k):
                        wo_copy(1, k).start()

                @pl.when(jnp.logical_and(corner, hop == hops - 2))
                def _():
                    first = c + c // 2
                    wo_range(first, first + 1 + lax.rem(c, 2))

                @pl.loop(0, 2)
                def _(way):
                    @pl.when(jnp.logical_or(jnp.logical_not(last), own_parity(way, c)))
                    def _():
                        compute(ring_member(jnp.where(way == 0, position - hop, position + hop), n), c)

        @pl.when(wave >= hops - 1)
        def _():
            project(wave - (hops - 1))

        @pl.when(wave >= hops - 1 + LAG)
        def _():
            attend(wave - (hops - 1) - LAG)

    @pl.loop(chunks - LAG, chunks)
    def _(c):
        attend(c)

    @pl.when(corner)
    def _():
        wo_range(early_pieces, 2 * pieces)

    slots = context.shape[0]
    parts = 2
    blocks = per_half // parts
    half_chunks = chunks // 2
    turns = parts * pieces

    def turn_of(i):
        first = i < turns // 2
        late = i - turns // 2
        part = jnp.where(first, i // (pieces // 2), lax.rem(late, parts))
        piece = jnp.where(first, lax.rem(i, pieces // 2), pieces // 2 + late // parts)
        return part, piece

    def term(group, part, k):
        start = pl.multiple_of((group * per_half + part * blocks) * rows, blocks * rows)
        total = jnp.zeros((blocks * rows, piece_width), jnp.float32)
        for s in range(slots):
            total += jnp.dot(
                context[s, pl.ds(start, blocks * rows)], w_half[k, s], preferred_element_type=jnp.float32
            )
        return total

    def mid_copy(i):
        return pltpu.make_async_remote_copy(
            src_ref=leaving.at[i], dst_ref=entering.at[i],
            send_sem=mid_send.at[i], recv_sem=mid_recv.at[i],
            device_id={"mp": opposite}, device_id_type=MESH,
        )

    def final_copy(i, part, k, b):
        return pltpu.make_async_remote_copy(
            src_ref=summed.at[i, b], dst_ref=final.at[x, k],
            send_sem=final_send.at[i, b], recv_sem=final_recv.at[x, k],
            device_id={"mp": half_first + part * blocks + b}, device_id_type=MESH,
        )

    def final_arrived(side, k):
        return pltpu.make_async_remote_copy(
            src_ref=final.at[side, k], dst_ref=final.at[side, k],
            send_sem=final_send.at[k, 0], recv_sem=final_recv.at[side, k],
            device_id={"mp": partner}, device_id_type=MESH,
        )

    def contexts_arrived(group, i):
        @pl.when(jnp.logical_or(i == 0, i == pieces // 2))
        def _():
            first = group * half_chunks + jnp.where(i == 0, 0, half_chunks - 1)
            for s in range(slots):
                @pl.when(slot != s)
                def _():
                    @pl.loop(first, jnp.where(i == 0, first + half_chunks - 1, first + 1))
                    def _(c):
                        context_arrived(s, c).wait_recv()

    @pl.when(inner)
    def _():
        @pl.loop(0, turns + LEAD)
        def _(i):
            @pl.when(i < turns)
            def _():
                part, k = turn_of(i)

                @pl.when(jnp.where(i < turns // 2, i < pieces // 2, part == 0))
                def _():
                    wo_own_copy(k).wait()
                    for s in range(slots):
                        @pl.when(slot != s)
                        def _():
                            wo_arrived(s, k).wait_recv()
                contexts_arrived(1 - half, i)
                leaving[i] = term(1 - half, part, k).astype(jnp.bfloat16)
                mid_copy(i).start()

            @pl.when(i >= LEAD)
            def _():
                j = i - LEAD
                part, k = turn_of(j)
                contexts_arrived(half, j)
                value = term(half, part, k)
                mid_copy(j).wait_recv()
                value = value + entering[j].astype(jnp.float32)
                summed[j] = value.astype(jnp.bfloat16).reshape(blocks, rows, piece_width)
                for b in range(blocks):
                    @pl.when(half_first + part * blocks + b != me)
                    def _():
                        final_copy(j, part, k, b).start()

                    @pl.when(half_first + part * blocks + b == me)
                    def _():
                        final[x, k] = summed[j, b]

    @pl.loop(0, pieces)
    def _(k):
        for side in range(2):
            @pl.when(jnp.logical_or(corner, x != side))
            def _():
                final_arrived(side, k).wait_recv()
            start = side * (pieces * piece_width) + k * piece_width
            columns = pl.ds(pl.multiple_of(start, piece_width), piece_width)
            within_block = pl.ds(pl.multiple_of(lax.rem(start, width), piece_width), piece_width)
            value = final[side, k]
            attended_ref[:, columns] = value
            stream_ref[:, columns] = (
                x_all[start // width, pl.ds(pl.multiple_of(me * rows, rows), rows), within_block].astype(jnp.float32) + value.astype(jnp.float32)
            ).astype(jnp.bfloat16)

    for c in range(chunks):
        shift_copy(c).wait_send()

    @pl.loop(0, chunks)
    def _(c):
        for step in range(1, n):
            kv_copy(c, step).wait_send()

        @pl.when(corner)
        def _():
            context_copy(0, c).wait_send()
        context_copy(1, c).wait_send()

    @pl.loop(0, hops * chunks)
    def _(i):
        hop = i // chunks + 1
        c = lax.rem(i, chunks)
        for way in range(2):
            @pl.when(sends(way, hop, c))
            def _():
                ring_copy(way, hop, c).wait_send()

    @pl.loop(0, pieces)
    def _(k):
        wo_copy(1, k).wait_send()

        @pl.when(corner)
        def _():
            wo_copy(0, k).wait_send()

    @pl.when(inner)
    def _():
        @pl.loop(0, turns)
        def _(i):
            part, k = turn_of(i)
            mid_copy(i).wait_send()
            for b in range(blocks):
                @pl.when(half_first + part * blocks + b != me)
                def _():
                    final_copy(i, part, k, b).wait_send()

    @pl.when(inner)
    def _():
        for c in range(chunks):
            short_copy(0, c).wait_send()

            @pl.when(own_parity(out_way, c))
            def _():
                short_copy(1, c).wait_send()


def rotary_tables(length):
    pair = (np.arange(HD) // 2).astype(np.float32)
    frequency = np.exp(pair * np.float32(-2.0 * math.log(ROPE_BASE) / HD)).astype(np.float32)
    angles = frequency[None, :] * np.arange(length, dtype=np.float32)[:, None]
    sign = np.where(np.arange(HD) % 2 == 0, -1.0, 1.0).astype(np.float32)
    return np.stack([np.cos(angles), np.sin(angles) * sign]).astype(np.float32)


def local(arriving, norm_gain, w_query, w_key, w_value, w_out):
    n = lax.axis_size("mp")
    length, width = arriving.shape[1:]
    rows = length // n
    full = n * width
    chunks = 8 if n <= 8 else 2
    pieces = 4 if n <= 8 else 2
    qw, kw, vw = w_query.shape[1], w_key.shape[1], w_value.shape[1]
    tables = rotary_tables(length)
    vmem = pl.BlockSpec(memory_space=pltpu.VMEM)
    hbm = pl.BlockSpec(memory_space=pltpu.HBM)
    bf16, f32 = jnp.bfloat16, jnp.float32
    dma = pltpu.SemaphoreType.DMA
    if n == 8:
        pieces = 8
        piece_width = full // (2 * pieces)
        per = 128
        chunks = length // per
        per_head = kw // KV_HEADS
        blocks = n // 4
        kernel = grid_kernel
        operands = (
            arriving[0],
            norm_gain[0].reshape(n, 1, width),
            w_query[0], w_key[0], w_value[0], w_out[0], jnp.asarray(tables.reshape(2, chunks, per, HD)),
        )
        scratch = [
            pltpu.VMEM((length, width), bf16),
            pltpu.VMEM((n, 1, width), bf16),
            pltpu.VMEM((2, chunks, per, HD), f32),
            pltpu.VMEM((n, length, width), bf16),
            pltpu.VMEM((n, qw + kw + vw, width), bf16),
            pltpu.VMEM((chunks, per, qw + kw + vw), f32),
            pltpu.VMEM((chunks, per, 128), f32),
            pltpu.VMEM((2, chunks, per, kw), f32),
            pltpu.VMEM((chunks, KV_HEADS, 2, per_head, per), bf16),
            pltpu.VMEM((chunks, n, 2, per_head, per), bf16),
            pltpu.VMEM((HD, length), bf16),
            pltpu.VMEM((HD, length), bf16),
            pltpu.VMEM((chunks, per, qw), bf16),
            pltpu.VMEM((4, length, qw), bf16),
            pltpu.VMEM((pieces, 4, qw, piece_width), bf16),
            pltpu.VMEM((2 * pieces, blocks * rows, piece_width), bf16),
            pltpu.VMEM((2 * pieces, blocks * rows, piece_width), bf16),
            pltpu.VMEM((2 * pieces, blocks, rows, piece_width), bf16),
            pltpu.VMEM((2, pieces, rows, piece_width), bf16),
            dma(()),
            dma(()),
            dma(()),
            dma((n, 3)),
            dma((chunks,)),
            dma((chunks,)),
            dma((2, n // 2, chunks)),
            dma((2, n // 2, chunks)),
            dma((2, chunks)),
            dma((chunks, n - 1)),
            dma((chunks, n - 1)),
            dma((pieces,)),
            dma((2, pieces)),
            dma((4, pieces)),
            dma((2, chunks)),
            dma((4, chunks)),
            dma((2 * pieces,)),
            dma((2 * pieces,)),
            dma((2 * pieces, blocks)),
            dma((2, pieces)),
        ]
    else:
        kernel = ring_kernel
        operands = (
            arriving[0].reshape(n, rows, width),
            norm_gain[0].reshape(n, 1, width),
            w_query[0], w_key[0], w_value[0], w_out[0], jnp.asarray(tables),
        )
        scratch = [
            pltpu.VMEM((n, rows, width), bf16),
            pltpu.VMEM((n, 1, width), bf16),
            pltpu.VMEM((2, length, HD), f32),
            pltpu.VMEM((n, n, rows, width), bf16),
            pltpu.VMEM((n, qw + kw + vw, width), bf16),
            pltpu.VMEM((chunks, length // chunks, qw + kw + vw), f32),
            pltpu.VMEM((chunks, length // chunks, 128), f32),
            pltpu.VMEM((KV_HEADS, 2, kw // KV_HEADS, length), bf16),
            pltpu.VMEM((n, 2, kw // KV_HEADS, length), bf16),
            pltpu.VMEM((2, HD, length), f32),
            pltpu.VMEM((HD, length), bf16),
            pltpu.VMEM((HD, length), bf16),
            pltpu.VMEM((n, rows, qw), bf16),
            pltpu.VMEM((qw, full), bf16),
            pltpu.VMEM((n, rows, qw), bf16),
            pltpu.VMEM((2, n, pieces, rows, full // (2 * pieces)), bf16),
            dma(()),
            dma(()),
            dma(()),
            dma((n, 3)),
            dma(()),
            dma((chunks,)),
            dma((chunks,)),
            dma((2, n // 2, chunks)),
            dma((2, n // 2, chunks)),
            dma((2, n - 1)),
            dma((2, n - 1)),
            dma((2, n - 1, pieces)),
            dma((2, n - 1, pieces)),
        ]
    attended, stream = pl.pallas_call(
        functools.partial(kernel, n, chunks, pieces),
        name="layer",
        out_shape=(pltpu.VMEM((rows, full), bf16),) * 2,
        in_specs=[hbm] * 7,
        out_specs=(vmem, vmem),
        scratch_shapes=scratch,
        compiler_params=pltpu.CompilerParams(collective_id=0, has_side_effects=True, vmem_limit_bytes=VMEM_LIMIT),
    )(*operands)
    return (attended[None], stream[None])


def solution(mesh):
    return jax.shard_map(
        local,
        mesh=mesh,
        in_specs=(
            P("section", None, "mp"),
            P("section", None),
            P("section", "mp", None),
            P("section", "mp", None),
            P("section", "mp", None),
            P("section", "mp", None),
        ),
        out_specs=(P("section", "mp", None), P("section", "mp", None)),
        check_vma=False,
    )
```

```python
import functools
import math

import jax
import jax.numpy as jnp
import numpy as np
from jax import lax
from jax.experimental import pallas as pl
from jax.experimental.pallas import tpu as pltpu
from jax.sharding import PartitionSpec as P

HD = 128
KV_HEADS = 8
ROPE_BASE = 500000.0
NORM_EPS = 1e-05
MESH = pl.DeviceIdType.MESH
VMEM_LIMIT = 63500000
AHEAD = 2
LEAD = 4
LAST = 2
EARLY_CORNER = 8
EARLY_INNER = 4


def ring_position(member, n):
    return jnp.where(member % 2 == 0, member // 2, n - 1 - member // 2)


def ring_member(position, n):
    position = lax.rem(position + 2 * n, n)
    return jnp.where(position < n // 2, 2 * position, 2 * (n - 1 - position) + 1)


def swap_pairs(x):
    lane = lax.broadcasted_iota(jnp.int32, x.shape, 1)
    width = x.shape[1]
    return jnp.where(lane % 2 == 0, pltpu.roll(x, width - 1, 1), pltpu.roll(x, 1, 1))


def ring_kernel(
    n, chunks, pieces, arriving, gain_hbm, wq, wk, wv, w_hbm, tables_hbm,
    attended_ref, stream_ref,
    staged, gain, tables, x_all, weights, acc, squares, sent, got, heads_kv, key_head, value_head, q_ref, w_out, context, running,
    stage_sem, gain_sem, tables_sem, w_sem, wo_sem, shift_send, shift_recv, ring_send, ring_recv, kv_send, kv_recv, send_sem, recv_sem,
):
    sections = lax.axis_size("section")
    section = lax.axis_index("section")
    me = lax.axis_index("mp")
    position = ring_position(me, n)
    right, left = ring_member(position + 1, n), ring_member(position - 1, n)
    following, previous = lax.rem(section + 1, sections), lax.rem(section + sections - 1, sections)
    hops = n // 2
    per = n // chunks
    rows, width = x_all.shape[2:]
    length = n * rows
    chunk_rows = per * rows
    qw, kw, vw = wq.shape[0], wk.shape[0], wv.shape[0]
    heads = qw // HD
    group_size = heads * n // KV_HEADS
    nn = (((1,), (0,)), ((), ()))
    nt = (((1,), (1,)), ((), ()))

    stage = pltpu.make_async_copy(arriving, staged, stage_sem)
    stage.start()
    gain_copy = pltpu.make_async_copy(gain_hbm, gain, gain_sem)
    gain_copy.start()
    tables_copy = pltpu.make_async_copy(tables_hbm, tables, tables_sem)
    tables_copy.start()
    barrier = pltpu.get_barrier_semaphore()
    for step in range(1, n):
        pl.semaphore_signal(barrier, inc=1, device_id={"mp": lax.rem(me + step, n)}, device_id_type=MESH)
    for partner in (following, previous):
        pl.semaphore_signal(barrier, inc=1, device_id={"section": partner}, device_id_type=MESH)

    def weight_copy(j, part):
        src, start, size = ((wq, 0, qw), (wk, qw, kw), (wv, qw + kw, vw))[part]
        return pltpu.make_async_copy(
            src.at[:, pl.ds(j * width, width)], weights.at[j, pl.ds(start, size)], w_sem.at[j, part]
        )

    def shift_copy(c):
        return pltpu.make_async_remote_copy(
            src_ref=staged.at[pl.ds(c * per, per)],
            dst_ref=x_all.at[me, pl.ds(c * per, per)],
            send_sem=shift_send.at[c], recv_sem=shift_recv.at[c],
            device_id={"section": following}, device_id_type=MESH,
        )

    def ring_copy(way, hop, c):
        origin = ring_member(position - (hop - 1) if way == 0 else position + (hop - 1), n)
        return pltpu.make_async_remote_copy(
            src_ref=x_all.at[origin, pl.ds(c * per, per)],
            dst_ref=x_all.at[origin, pl.ds(c * per, per)],
            send_sem=ring_send.at[way, hop - 1, c], recv_sem=ring_recv.at[way, hop - 1, c],
            device_id={"mp": right if way == 0 else left}, device_id_type=MESH,
        )

    for j in range(n):
        for part in range(3):
            weight_copy(j, part).start()
    stage.wait()
    pl.semaphore_wait(barrier, n + 1)
    for c in range(chunks):
        shift_copy(c).start()
    acc[...] = jnp.zeros_like(acc)
    squares[...] = jnp.zeros_like(squares)

    def compute(slot, c):
        x = x_all[slot, pl.ds(c * per, per)].astype(jnp.float32).reshape(chunk_rows, width)
        total = x[:, :128] * x[:, :128]
        for g in range(1, width // 128):
            part = x[:, g * 128 : (g + 1) * 128]
            total = total + part * part
        squares[c] += total
        scaled = (x * gain[slot].astype(jnp.float32)).astype(jnp.bfloat16)
        acc[c] += lax.dot_general(scaled, weights[slot], nt, preferred_element_type=jnp.float32)

    for c in range(chunks):
        shift_copy(c).wait_recv()
        ring_copy(0, 1, c).start()
        ring_copy(1, 1, c).start()
    for j in range(n):
        for part in range(3):
            weight_copy(j, part).wait()
    gain_copy.wait()
    tables_copy.wait()
    wo_copy = pltpu.make_async_copy(w_hbm, w_out, wo_sem)
    wo_copy.start()

    @pl.loop(0, chunks)
    def _(c):
        compute(me, c)

    cos, sin = tables[0], tables[1]
    lane = lax.broadcasted_iota(jnp.int32, (HD, kw), 1)
    source = lax.broadcasted_iota(jnp.int32, (HD, kw), 0)
    pick = (source == (me * kw + lane) // (2 * KV_HEADS) * 2 + lane % 2).astype(jnp.float32)
    k_cos = lax.dot_general(cos, pick, nn, precision=lax.Precision.HIGHEST, preferred_element_type=jnp.float32)
    k_sin = lax.dot_general(sin, pick, nn, precision=lax.Precision.HIGHEST, preferred_element_type=jnp.float32)
    per_head = kw // KV_HEADS
    target = lax.broadcasted_iota(jnp.int32, (kw, kw), 0)
    origin_row = lax.broadcasted_iota(jnp.int32, (kw, kw), 1)
    head, within = target // per_head, target % per_head
    order = (origin_row == (within // 2 * KV_HEADS + head) * 2 + within % 2).astype(jnp.bfloat16)

    @pl.loop(0, hops * chunks)
    def _(i):
        hop = i // chunks + 1
        turn = lax.rem(i, chunks)
        last = hop == hops
        c = jnp.where(last, turn // 2 + lax.rem(turn, 2) * (chunks // 2), turn)
        low = c < chunks // 2
        for way in range(2):
            mine = low if way == 0 else jnp.logical_not(low)

            @pl.when(jnp.logical_or(jnp.logical_not(last), mine))
            def _():
                ring_copy(way, hop, c).wait_recv()

            @pl.when(jnp.logical_and(hop < hops, jnp.logical_or(hop + 1 < hops, mine)))
            def _():
                ring_copy(way, hop + 1, c).start()

        @pl.loop(0, 2)
        def _(way):
            mine = low == (way == 0)

            @pl.when(jnp.logical_or(jnp.logical_not(last), mine))
            def _():
                compute(ring_member(jnp.where(way == 0, position - hop, position + hop), n), c)

    inverse = lax.rsqrt(
        jnp.sum(squares[...].reshape(length, 128), axis=1, keepdims=True) * (1.0 / (n * width)) + NORM_EPS
    )
    k = acc[:, :, qw : qw + kw].reshape(length, kw) * inverse
    k_rot = (k * k_cos + swap_pairs(k) * k_sin).astype(jnp.bfloat16)
    def kv_copy(part, step):
        other = lax.rem(me + step, n)
        return pltpu.make_async_remote_copy(
            src_ref=sent.at[other * heads // group_size, part], dst_ref=got.at[me, part],
            send_sem=kv_send.at[part, step - 1], recv_sem=kv_recv.at[part, step - 1],
            device_id={"mp": other}, device_id_type=MESH,
        )

    def order_and_send(part, channels):
        ordered = lax.dot_general(order, channels, nt, preferred_element_type=jnp.float32)
        for h in range(KV_HEADS):
            sent[h, part] = ordered[h * per_head : (h + 1) * per_head].astype(jnp.bfloat16)
        for step in range(1, n):
            kv_copy(part, step).start()

    order_and_send(0, k_rot)
    order_and_send(1, (acc[:, :, qw + kw :].reshape(length, vw) * inverse).astype(jnp.bfloat16))
    got[me] = sent[me * heads // group_size]
    for h in range(heads):
        q = acc[:, :, h * HD : (h + 1) * HD].reshape(length, HD) * inverse
        q_ref[:, :, h * HD : (h + 1) * HD] = (
            (q * cos + swap_pairs(q) * sin).reshape(n, rows, HD).astype(jnp.bfloat16)
        )

    def receive(part, whole):
        for step in range(1, n):
            kv_copy(part, step).wait_recv()
        for j in range(n):
            heads_kv[part, j * per_head : (j + 1) * per_head] = got[j, part].astype(jnp.float32)
        whole[...] = heads_kv[part].astype(jnp.bfloat16)

    receive(0, key_head)

    piece_width = running.shape[4]
    scale = 1.0 / math.sqrt(HD)

    def attend(block, ready=None):
        row = lax.broadcasted_iota(jnp.int32, (rows, length), 0) + block * rows
        column = lax.broadcasted_iota(jnp.int32, (rows, length), 1)
        probs = []
        for h in range(heads):
            q = q_ref[block, :, h * HD : (h + 1) * HD]
            scores = lax.dot_general(q, key_head[...], nn, preferred_element_type=jnp.float32) * scale
            scores = jnp.where(row >= column, scores, -1e30)
            exponent = jnp.exp(scores - jnp.max(scores, axis=1, keepdims=True))
            probs.append((exponent / jnp.sum(exponent, axis=1, keepdims=True)).astype(jnp.bfloat16))
        if ready is not None:
            ready()
        for h in range(heads):
            context[block, :, h * HD : (h + 1) * HD] = lax.dot_general(
                probs[h], value_head[...], nt, preferred_element_type=jnp.float32
            ).astype(jnp.bfloat16)

    def block_of(way, step):
        return ring_member(position - 1 - step if way == 0 else position + 1 + step, n)

    def term(way, step, piece):
        start = (way * pieces + piece) * piece_width
        return jnp.dot(
            context[block_of(way, step)], w_out[:, start : start + piece_width], preferred_element_type=jnp.float32
        )

    def sum_copy(way, step, piece):
        return pltpu.make_async_remote_copy(
            src_ref=running.at[way, step, piece],
            dst_ref=running.at[way, step + 1, piece],
            send_sem=send_sem.at[way, step, piece], recv_sem=recv_sem.at[way, step, piece],
            device_id={"mp": right if way == 0 else left}, device_id_type=MESH,
        )

    wo_copy.wait()
    for way in range(2):
        attend(block_of(way, 0), functools.partial(receive, 1, value_head) if way == 0 else None)
        for piece in range(pieces):
            running[way, 0, piece] = term(way, 0, piece).astype(jnp.bfloat16)
            sum_copy(way, 0, piece).start()

    def ahead(step):
        @pl.when(step < n // 2)
        def _():
            attend(block_of(0, step))
            attend(block_of(1, step))

        @pl.when(step == n // 2)
        def _():
            attend(me)

    ahead(1)

    @pl.loop(1, n - 1)
    def _(step):
        for piece in range(pieces):
            for way in range(2):
                value = term(way, step, piece)
                sum_copy(way, step - 1, piece).wait_recv()
                running[way, step, piece] = (running[way, step, piece].astype(jnp.float32) + value).astype(jnp.bfloat16)
                sum_copy(way, step, piece).start()
        ahead(step + 1)

    for j in range(n):
        stream_ref[:, j * width : (j + 1) * width] = x_all[j, me]
    for piece in range(pieces):
        for way in range(2):
            value = term(way, n - 1, piece)
            sum_copy(way, n - 2, piece).wait_recv()
            value = running[way, n - 1, piece].astype(jnp.float32) + value
            columns = slice((way * pieces + piece) * piece_width, (way * pieces + piece + 1) * piece_width)
            attended_ref[:, columns] = value.astype(jnp.bfloat16)
            stream_ref[:, columns] = (stream_ref[:, columns].astype(jnp.float32) + value).astype(jnp.bfloat16)

    for c in range(chunks):
        shift_copy(c).wait_send()
    for part in range(2):
        for step in range(1, n):
            kv_copy(part, step).wait_send()

    @pl.loop(0, hops * chunks)
    def _(i):
        hop = i // chunks + 1
        c = lax.rem(i, chunks)
        for way in range(2):
            mine = (c < chunks // 2) if way == 0 else (c >= chunks // 2)

            @pl.when(jnp.logical_or(hop < hops, mine))
            def _():
                ring_copy(way, hop, c).wait_send()

    @pl.loop(0, n - 1)
    def _(step):
        for piece in range(pieces):
            for way in range(2):
                sum_copy(way, step, piece).wait_send()


def grid_kernel(
    n, chunks, pieces, arriving, gain_hbm, wq, wk, wv, w_hbm, tables_hbm,
    attended_ref, stream_ref,
    staged, gain, tables, x_all, weights, acc, squares, rotary, sent, got, key_head, value_head, q_ref,
    context, w_half, leaving, entering, summed, final,
    stage_sem, gain_sem, tables_sem, w_sem, shift_send, shift_recv, ring_send, ring_recv, short_send, kv_send, kv_recv,
    wo_own, wo_send, wo_recv, context_send, context_recv, mid_send, mid_recv, final_send, final_recv,
):
    sections = lax.axis_size("section")
    section = lax.axis_index("section")
    me = lax.axis_index("mp")
    position = ring_position(me, n)
    right, left = ring_member(position + 1, n), ring_member(position - 1, n)
    following, previous = lax.rem(section + 1, sections), lax.rem(section + sections - 1, sections)
    hops = n // 2
    rows = attended_ref.shape[0]
    length, width = x_all.shape[1:]
    per = length // chunks
    qw, kw, vw = wq.shape[0], wk.shape[0], wv.shape[0]
    heads = qw // HD
    group_size = heads * n // KV_HEADS
    nn = (((1,), (0,)), ((), ()))
    nt = (((1,), (1,)), ((), ()))

    def part_of(c):
        return pl.ds(pl.multiple_of(c * per, per), per)

    z, x = me // 2, lax.rem(me, 2)
    half = z // 2
    inner_row = 1 + half
    inner = z == inner_row
    corner = jnp.logical_not(inner)
    out_way = lax.rem(position, 2)
    partner = 2 * z + 1 - x
    opposite = 2 * (2 - half) + x
    beyond = ring_member(jnp.where(out_way == 1, position + 1, position - 1), n)
    slot = jnp.where(inner, 2, 0) + x
    per_half = n // 2
    half_first = half * per_half

    stage = pltpu.make_async_copy(arriving, staged, stage_sem)
    stage.start()
    gain_copy = pltpu.make_async_copy(gain_hbm, gain, gain_sem)
    gain_copy.start()
    tables_copy = pltpu.make_async_copy(tables_hbm, tables, tables_sem)
    tables_copy.start()
    barrier = pltpu.get_barrier_semaphore()
    for step in range(1, n):
        pl.semaphore_signal(barrier, inc=1, device_id={"mp": lax.rem(me + step, n)}, device_id_type=MESH)
    for partner_section in (following, previous):
        pl.semaphore_signal(barrier, inc=1, device_id={"section": partner_section}, device_id_type=MESH)

    def weight_copy(j, part):
        src, start, size = ((wq, 0, qw), (wk, qw, kw), (wv, qw + kw, vw))[part]
        return pltpu.make_async_copy(
            src.at[:, pl.ds(j * width, width)], weights.at[j, pl.ds(start, size)], w_sem.at[j, part]
        )

    def shift_copy(c):
        return pltpu.make_async_remote_copy(
            src_ref=staged.at[part_of(c)],
            dst_ref=x_all.at[me, part_of(c)],
            send_sem=shift_send.at[c], recv_sem=shift_recv.at[c],
            device_id={"section": following}, device_id_type=MESH,
        )

    def share_of(way, c):
        return pl.ds(pl.multiple_of(c * per + way * (per // 2), per // 2), per // 2)

    def ring_copy(way, hop, c, shared):
        origin = ring_member(position - (hop - 1) if way == 0 else position + (hop - 1), n)
        tokens = share_of(way, c) if shared else part_of(c)
        return pltpu.make_async_remote_copy(
            src_ref=x_all.at[origin, tokens], dst_ref=x_all.at[origin, tokens],
            send_sem=ring_send.at[way, hop - 1, c], recv_sem=ring_recv.at[way, hop - 1, c],
            device_id={"mp": right if way == 0 else left}, device_id_type=MESH,
        )

    def short_copy(late, c):
        origin = beyond if late else me
        tokens = share_of(out_way, c) if late else part_of(c)
        return pltpu.make_async_remote_copy(
            src_ref=x_all.at[origin, tokens], dst_ref=x_all.at[origin, tokens],
            send_sem=short_send.at[late, c], recv_sem=ring_recv.at[out_way, hops - 2 + late, c],
            device_id={"mp": partner}, device_id_type=MESH,
        )

    def through(way):
        return jnp.logical_or(inner, out_way != way)

    piece_width = w_half.shape[3]

    def wo_source(target, k):
        owner = jnp.where(target == 0, x, 1 - x)
        start = pl.multiple_of(owner * (pieces * piece_width) + k * piece_width, piece_width)
        return w_hbm.at[:, pl.ds(start, piece_width)], 2 * inner_row + owner

    def wo_copy(target, k):
        src, device = wo_source(target, k)
        return pltpu.make_async_remote_copy(
            src_ref=src, dst_ref=w_half.at[k, slot],
            send_sem=wo_send.at[target, k], recv_sem=wo_recv.at[slot, k],
            device_id={"mp": device}, device_id_type=MESH,
        )

    def wo_own_copy(k):
        src, _ = wo_source(0, k)
        return pltpu.make_async_copy(src, w_half.at[k, slot], wo_own.at[k])

    def wo_arrived(s, k):
        return pltpu.make_async_remote_copy(
            src_ref=w_half.at[k, s], dst_ref=w_half.at[k, s],
            send_sem=wo_send.at[0, k], recv_sem=wo_recv.at[s, k],
            device_id={"mp": partner}, device_id_type=MESH,
        )

    for j in range(n):
        for part in range(3):
            weight_copy(j, part).start()
    stage.wait()
    pl.semaphore_wait(barrier, n + 1)
    for c in range(chunks):
        shift_copy(c).start()
    acc[...] = jnp.zeros_like(acc)
    squares[...] = jnp.zeros_like(squares)
    key_head[...] = jnp.zeros_like(key_head)
    value_head[...] = jnp.zeros_like(value_head)

    def compute(source, c):
        block = x_all[source, part_of(c)].astype(jnp.float32)
        total = block[:, :128] * block[:, :128]
        for g in range(1, width // 128):
            part = block[:, g * 128 : (g + 1) * 128]
            total = total + part * part
        squares[c] += total
        scaled = (block * gain[source].astype(jnp.float32)).astype(jnp.bfloat16)
        acc[c] += lax.dot_general(scaled, weights[source], nt, preferred_element_type=jnp.float32)

    def start_own(c):
        shift_copy(c).wait_recv()
        ring_copy(0, 1, c, False).start()
        ring_copy(1, 1, c, False).start()

        @pl.when(inner)
        def _():
            short_copy(0, c).start()

    for c in range(AHEAD):
        start_own(c)
    for j in range(n):
        for part in range(3):
            weight_copy(j, part).wait()
    gain_copy.wait()
    tables_copy.wait()

    @pl.when(inner)
    def _():
        @pl.loop(0, pieces)
        def _(k):
            wo_own_copy(k).start()

    lane = lax.broadcasted_iota(jnp.int32, (HD, kw), 1)
    source = lax.broadcasted_iota(jnp.int32, (HD, kw), 0)
    pick = (source == (me * kw + lane) // (2 * KV_HEADS) * 2 + lane % 2).astype(jnp.float32)
    for t in range(2):
        picked = lax.dot_general(
            tables[t].reshape(length, HD), pick, nn, precision=lax.Precision.HIGHEST, preferred_element_type=jnp.float32
        )
        rotary[t] = picked.reshape(chunks, per, kw)
    per_head = kw // KV_HEADS
    target = lax.broadcasted_iota(jnp.int32, (kw, kw), 0)
    origin_row = lax.broadcasted_iota(jnp.int32, (kw, kw), 1)
    head, within = target // per_head, target % per_head
    order = (origin_row == (within // 2 * KV_HEADS + head) * 2 + within % 2).astype(jnp.bfloat16)

    def kv_copy(c, step):
        other = lax.rem(me + step, n)
        return pltpu.make_async_remote_copy(
            src_ref=sent.at[c, other * heads // group_size], dst_ref=got.at[c, me],
            send_sem=kv_send.at[c, step - 1], recv_sem=kv_recv.at[c, step - 1],
            device_id={"mp": other}, device_id_type=MESH,
        )

    def project(c):
        inverse = lax.rsqrt(jnp.sum(squares[c], axis=1, keepdims=True) * (1.0 / (n * width)) + NORM_EPS)
        k = acc[c, :, qw : qw + kw] * inverse
        k_rot = (k * rotary[0, c] + swap_pairs(k) * rotary[1, c]).astype(jnp.bfloat16)
        v = (acc[c, :, qw + kw :] * inverse).astype(jnp.bfloat16)
        for part, channels in enumerate((k_rot, v)):
            ordered = lax.dot_general(order, channels, nt, preferred_element_type=jnp.float32)
            for h in range(KV_HEADS):
                sent[c, h, part] = ordered[h * per_head : (h + 1) * per_head].astype(jnp.bfloat16)
        for step in range(1, n):
            kv_copy(c, step).start()
        got[c, me] = sent[c, me * heads // group_size]
        for h in range(heads):
            q = acc[c, :, h * HD : (h + 1) * HD] * inverse
            q_ref[c, :, h * HD : (h + 1) * HD] = (q * tables[0, c] + swap_pairs(q) * tables[1, c]).astype(jnp.bfloat16)

    scale = 1.0 / (math.sqrt(HD) * math.log(2.0))

    def attend(c):
        for step in range(1, n):
            kv_copy(c, step).wait_recv()
        for j in range(n):
            key_head[j * per_head : (j + 1) * per_head, part_of(c)] = got[c, j, 0]
            value_head[j * per_head : (j + 1) * per_head, part_of(c)] = got[c, j, 1]
        row = lax.broadcasted_iota(jnp.int32, (per, length), 0) + c * per
        column = lax.broadcasted_iota(jnp.int32, (per, length), 1)
        for h in range(heads):
            q = q_ref[c, :, h * HD : (h + 1) * HD]
            scores = lax.dot_general(q, key_head[...], nn, preferred_element_type=jnp.float32)
            scores = jnp.where(row >= column, scores, -1e30)
            exponent = jnp.exp2((scores - jnp.max(scores, axis=1, keepdims=True)) * scale)
            probs = (exponent * (1.0 / jnp.sum(exponent, axis=1, keepdims=True))).astype(jnp.bfloat16)
            context[slot, part_of(c), h * HD : (h + 1) * HD] = lax.dot_general(
                probs, value_head[...], nt, preferred_element_type=jnp.float32
            ).astype(jnp.bfloat16)

        @pl.when(corner)
        def _():
            context_copy(0, c).start()

        context_copy(1, c).start()

    def context_copy(target, c):
        return pltpu.make_async_remote_copy(
            src_ref=context.at[slot, part_of(c)], dst_ref=context.at[slot, part_of(c)],
            send_sem=context_send.at[target, c], recv_sem=context_recv.at[slot, c],
            device_id={"mp": 2 * inner_row + (x if target == 0 else 1 - x)}, device_id_type=MESH,
        )

    def context_arrived(s, c):
        return pltpu.make_async_remote_copy(
            src_ref=context.at[s, part_of(c)], dst_ref=context.at[s, part_of(c)],
            send_sem=context_send.at[0, c], recv_sem=context_recv.at[s, c],
            device_id={"mp": partner}, device_id_type=MESH,
        )

    def wo_range(first, last):
        @pl.loop(first, last)
        def _(i):
            wo_copy(lax.rem(i, 2), i // 2).start()

    @pl.loop(0, chunks + hops - 1)
    def _(wave):
        @pl.when(wave + AHEAD < chunks)
        def _():
            start_own(wave + AHEAD)

        @pl.when(wave < chunks)
        def _():
            compute(me, wave)

        @pl.when(jnp.logical_and(wave > hops, wave < chunks + hops - 2))
        def _():
            attend(wave - hops - 1)

        @pl.loop(1, hops + 1)
        def _(hop):
            c = wave - (hop - 1)
            last = hop == hops

            @pl.when(jnp.logical_and(c >= 0, c < chunks))
            def _():
                for way in range(2):
                    @pl.when(jnp.logical_not(last))
                    def _():
                        ring_copy(way, hop, c, False).wait_recv()

                    @pl.when(last)
                    def _():
                        ring_copy(way, hop, c, True).wait_recv()

                    @pl.when(jnp.logical_or(hop < hops - 2, jnp.logical_and(hop == hops - 2, through(way))))
                    def _():
                        ring_copy(way, hop + 1, c, False).start()

                    @pl.when(jnp.logical_and(hop == hops - 1, through(way)))
                    def _():
                        ring_copy(way, hop + 1, c, True).start()

                    @pl.when(jnp.logical_and(jnp.logical_and(inner, out_way == way), hop == 1))
                    def _():
                        short_copy(1, c).start()

                @pl.when(jnp.logical_and(inner, hop == hops - 2))
                def _():
                    @pl.loop(c * EARLY_INNER // chunks, (c + 1) * EARLY_INNER // chunks)
                    def _(k):
                        wo_copy(1, k).start()

                @pl.when(jnp.logical_and(corner, hop == hops - 2))
                def _():
                    wo_range(c * EARLY_CORNER // chunks, (c + 1) * EARLY_CORNER // chunks)

                @pl.loop(0, jnp.where(last, 1, 2))
                def _(way):
                    compute(ring_member(jnp.where(way == 0, position - hop, position + hop), n), c)

                @pl.when(jnp.logical_and(c == chunks - 1, hop == hops - 1))
                def _():
                    attend(chunks - 3)

        @pl.when(wave >= hops - 1)
        def _():
            project(wave - (hops - 1))

    slots = context.shape[0]
    parts = per_half
    half_chunks = chunks // 2
    turns = parts * pieces

    def turn_of(i):
        first = i < turns // 2
        late = i - turns // 2
        part = jnp.where(first, i // (pieces // 2), lax.rem(late, parts))
        piece = jnp.where(first, lax.rem(i, pieces // 2), pieces // 2 + late // parts)
        return part, piece

    def term(group, part, k):
        start = pl.multiple_of((group * per_half + part) * rows, rows)
        total = jnp.zeros((rows, piece_width), jnp.float32)
        for s in range(slots):
            total += jnp.dot(
                context[s, pl.ds(start, rows)], w_half[k, s], preferred_element_type=jnp.float32
            )
        return total

    def mid_copy(i):
        return pltpu.make_async_remote_copy(
            src_ref=leaving.at[i], dst_ref=entering.at[i],
            send_sem=mid_send.at[i], recv_sem=mid_recv.at[i],
            device_id={"mp": opposite}, device_id_type=MESH,
        )

    def final_copy(i):
        part, k = turn_of(i)
        return pltpu.make_async_remote_copy(
            src_ref=summed.at[i], dst_ref=final.at[x, k],
            send_sem=final_send.at[i], recv_sem=final_recv.at[x, k],
            device_id={"mp": half_first + part}, device_id_type=MESH,
        )

    def final_arrived(side, k):
        return pltpu.make_async_remote_copy(
            src_ref=final.at[side, k], dst_ref=final.at[side, k],
            send_sem=final_send.at[k], recv_sem=final_recv.at[side, k],
            device_id={"mp": partner}, device_id_type=MESH,
        )

    def contexts_arrived(group, i):
        step = pieces // 2

        @pl.when(jnp.logical_and(lax.rem(i, step) == 0, i // step < half_chunks))
        def _():
            for s in range(slots):
                @pl.when(slot != s)
                def _():
                    context_arrived(s, group * half_chunks + i // step).wait_recv()

    @pl.loop(0, turns + LEAD)
    def _(i):
        @pl.when(jnp.logical_or(i == LAST - 1, i == LAST))
        def _():
            attend(chunks - 2 + i - (LAST - 1))

        @pl.when(jnp.logical_and(corner, i == LAST))
        def _():
            wo_range(EARLY_CORNER, 2 * pieces)

        @pl.when(inner)
        def _():
            @pl.when(i == LAST)
            def _():
                @pl.loop(EARLY_INNER, pieces)
                def _(k):
                    wo_copy(1, k).start()

            @pl.when(i < turns)
            def _():
                part, k = turn_of(i)

                @pl.when(jnp.where(i < turns // 2, i < pieces // 2, part == 0))
                def _():
                    wo_own_copy(k).wait()
                    for s in range(slots):
                        @pl.when(slot != s)
                        def _():
                            wo_arrived(s, k).wait_recv()
                contexts_arrived(1 - half, i)
                leaving[i] = term(1 - half, part, k).astype(jnp.bfloat16)
                mid_copy(i).start()

            @pl.when(i >= LEAD)
            def _():
                j = i - LEAD
                part, k = turn_of(j)
                contexts_arrived(half, j)
                value = term(half, part, k)
                mid_copy(j).wait_recv()
                value = value + entering[j].astype(jnp.float32)
                value = value.astype(jnp.bfloat16)

                @pl.when(half_first + part != me)
                def _():
                    summed[j] = value
                    final_copy(j).start()

                @pl.when(half_first + part == me)
                def _():
                    final[x, k] = value

    @pl.loop(0, pieces)
    def _(k):
        for side in range(2):
            @pl.when(jnp.logical_or(corner, x != side))
            def _():
                final_arrived(side, k).wait_recv()
            start = side * (pieces * piece_width) + k * piece_width
            columns = pl.ds(pl.multiple_of(start, piece_width), piece_width)
            within_block = pl.ds(pl.multiple_of(lax.rem(start, width), piece_width), piece_width)
            value = final[side, k]
            attended_ref[:, columns] = value
            stream_ref[:, columns] = (
                x_all[start // width, pl.ds(pl.multiple_of(me * rows, rows), rows), within_block].astype(jnp.float32) + value.astype(jnp.float32)
            ).astype(jnp.bfloat16)

    for c in range(chunks):
        shift_copy(c).wait_send()

    @pl.loop(0, chunks)
    def _(c):
        for step in range(1, n):
            kv_copy(c, step).wait_send()

        @pl.when(corner)
        def _():
            context_copy(0, c).wait_send()
        context_copy(1, c).wait_send()

    @pl.loop(0, chunks)
    def _(c):
        for way in range(2):
            @pl.loop(1, hops - 1)
            def _(hop):
                ring_copy(way, hop, c, False).wait_send()

            @pl.when(through(way))
            def _():
                ring_copy(way, hops - 1, c, False).wait_send()
                ring_copy(way, hops, c, True).wait_send()

    @pl.loop(0, pieces)
    def _(k):
        wo_copy(1, k).wait_send()

        @pl.when(corner)
        def _():
            wo_copy(0, k).wait_send()

    @pl.when(inner)
    def _():
        @pl.loop(0, turns)
        def _(i):
            part, k = turn_of(i)
            mid_copy(i).wait_send()

            @pl.when(half_first + part != me)
            def _():
                final_copy(i).wait_send()

    @pl.when(inner)
    def _():
        for c in range(chunks):
            short_copy(0, c).wait_send()
            short_copy(1, c).wait_send()


def rotary_tables(length):
    pair = (np.arange(HD) // 2).astype(np.float32)
    frequency = np.exp(pair * np.float32(-2.0 * math.log(ROPE_BASE) / HD)).astype(np.float32)
    angles = frequency[None, :] * np.arange(length, dtype=np.float32)[:, None]
    sign = np.where(np.arange(HD) % 2 == 0, -1.0, 1.0).astype(np.float32)
    return np.stack([np.cos(angles), np.sin(angles) * sign]).astype(np.float32)


def local(arriving, norm_gain, w_query, w_key, w_value, w_out):
    n = lax.axis_size("mp")
    length, width = arriving.shape[1:]
    rows = length // n
    full = n * width
    chunks = 8 if n <= 8 else 2
    pieces = 4 if n <= 8 else 2
    qw, kw, vw = w_query.shape[1], w_key.shape[1], w_value.shape[1]
    tables = rotary_tables(length)
    vmem = pl.BlockSpec(memory_space=pltpu.VMEM)
    hbm = pl.BlockSpec(memory_space=pltpu.HBM)
    bf16, f32 = jnp.bfloat16, jnp.float32
    dma = pltpu.SemaphoreType.DMA
    if n == 8:
        pieces = 8
        piece_width = full // (2 * pieces)
        per = 128
        chunks = length // per
        per_head = kw // KV_HEADS
        turns = n // 2 * pieces
        kernel = grid_kernel
        operands = (
            arriving[0],
            norm_gain[0].reshape(n, 1, width),
            w_query[0], w_key[0], w_value[0], w_out[0], jnp.asarray(tables.reshape(2, chunks, per, HD)),
        )
        scratch = [
            pltpu.VMEM((length, width), bf16),
            pltpu.VMEM((n, 1, width), bf16),
            pltpu.VMEM((2, chunks, per, HD), f32),
            pltpu.VMEM((n, length, width), bf16),
            pltpu.VMEM((n, qw + kw + vw, width), bf16),
            pltpu.VMEM((chunks, per, qw + kw + vw), f32),
            pltpu.VMEM((chunks, per, 128), f32),
            pltpu.VMEM((2, chunks, per, kw), f32),
            pltpu.VMEM((chunks, KV_HEADS, 2, per_head, per), bf16),
            pltpu.VMEM((chunks, n, 2, per_head, per), bf16),
            pltpu.VMEM((HD, length), bf16),
            pltpu.VMEM((HD, length), bf16),
            pltpu.VMEM((chunks, per, qw), bf16),
            pltpu.VMEM((4, length, qw), bf16),
            pltpu.VMEM((pieces, 4, qw, piece_width), bf16),
            pltpu.VMEM((turns, rows, piece_width), bf16),
            pltpu.VMEM((turns, rows, piece_width), bf16),
            pltpu.VMEM((turns, rows, piece_width), bf16),
            pltpu.VMEM((2, pieces, rows, piece_width), bf16),
            dma(()),
            dma(()),
            dma(()),
            dma((n, 3)),
            dma((chunks,)),
            dma((chunks,)),
            dma((2, n // 2, chunks)),
            dma((2, n // 2, chunks)),
            dma((2, chunks)),
            dma((chunks, n - 1)),
            dma((chunks, n - 1)),
            dma((pieces,)),
            dma((2, pieces)),
            dma((4, pieces)),
            dma((2, chunks)),
            dma((4, chunks)),
            dma((turns,)),
            dma((turns,)),
            dma((turns,)),
            dma((2, pieces)),
        ]
    else:
        kernel = ring_kernel
        operands = (
            arriving[0].reshape(n, rows, width),
            norm_gain[0].reshape(n, 1, width),
            w_query[0], w_key[0], w_value[0], w_out[0], jnp.asarray(tables),
        )
        scratch = [
            pltpu.VMEM((n, rows, width), bf16),
            pltpu.VMEM((n, 1, width), bf16),
            pltpu.VMEM((2, length, HD), f32),
            pltpu.VMEM((n, n, rows, width), bf16),
            pltpu.VMEM((n, qw + kw + vw, width), bf16),
            pltpu.VMEM((chunks, length // chunks, qw + kw + vw), f32),
            pltpu.VMEM((chunks, length // chunks, 128), f32),
            pltpu.VMEM((KV_HEADS, 2, kw // KV_HEADS, length), bf16),
            pltpu.VMEM((n, 2, kw // KV_HEADS, length), bf16),
            pltpu.VMEM((2, HD, length), f32),
            pltpu.VMEM((HD, length), bf16),
            pltpu.VMEM((HD, length), bf16),
            pltpu.VMEM((n, rows, qw), bf16),
            pltpu.VMEM((qw, full), bf16),
            pltpu.VMEM((n, rows, qw), bf16),
            pltpu.VMEM((2, n, pieces, rows, full // (2 * pieces)), bf16),
            dma(()),
            dma(()),
            dma(()),
            dma((n, 3)),
            dma(()),
            dma((chunks,)),
            dma((chunks,)),
            dma((2, n // 2, chunks)),
            dma((2, n // 2, chunks)),
            dma((2, n - 1)),
            dma((2, n - 1)),
            dma((2, n - 1, pieces)),
            dma((2, n - 1, pieces)),
        ]
    attended, stream = pl.pallas_call(
        functools.partial(kernel, n, chunks, pieces),
        name="layer",
        out_shape=(pltpu.VMEM((rows, full), bf16),) * 2,
        in_specs=[hbm] * 7,
        out_specs=(vmem, vmem),
        scratch_shapes=scratch,
        compiler_params=pltpu.CompilerParams(collective_id=0, has_side_effects=True, vmem_limit_bytes=VMEM_LIMIT),
    )(*operands)
    return (attended[None], stream[None])


def solution(mesh):
    return jax.shard_map(
        local,
        mesh=mesh,
        in_specs=(
            P("section", None, "mp"),
            P("section", None),
            P("section", "mp", None),
            P("section", "mp", None),
            P("section", "mp", None),
            P("section", "mp", None),
        ),
        out_specs=(P("section", "mp", None), P("section", "mp", None)),
        check_vma=False,
    )
```

```python
import functools
import math

import jax
import jax.numpy as jnp
import numpy as np
from jax import lax
from jax.experimental import pallas as pl
from jax.experimental.pallas import tpu as pltpu
from jax.sharding import PartitionSpec as P

HD = 128
KV_HEADS = 8
ROPE_BASE = 500000.0
NORM_EPS = 1e-05
MESH = pl.DeviceIdType.MESH
VMEM_LIMIT = 63500000
AHEAD = 2
LEAD = 4
FIRST = 2
START = 1
LAST = 3
SLOT_CORNER = 2
SLOT_INNER = 2
EARLY_CORNER = 7
EARLY_INNER = 5
MORE = 1
HEAD = 3


def ring_position(member, n):
    return jnp.where(member % 2 == 0, member // 2, n - 1 - member // 2)


def ring_member(position, n):
    position = lax.rem(position + 2 * n, n)
    return jnp.where(position < n // 2, 2 * position, 2 * (n - 1 - position) + 1)


def swap_pairs(x):
    lane = lax.broadcasted_iota(jnp.int32, x.shape, 1)
    width = x.shape[1]
    return jnp.where(lane % 2 == 0, pltpu.roll(x, width - 1, 1), pltpu.roll(x, 1, 1))


def ring_kernel(
    n, chunks, pieces, arriving, gain_hbm, wq, wk, wv, w_hbm, tables_hbm,
    attended_ref, stream_ref,
    staged, gain, tables, x_all, weights, acc, squares, sent, got, heads_kv, key_head, value_head, q_ref, w_out, context, running,
    stage_sem, gain_sem, tables_sem, w_sem, wo_sem, shift_send, shift_recv, ring_send, ring_recv, kv_send, kv_recv, send_sem, recv_sem,
):
    sections = lax.axis_size("section")
    section = lax.axis_index("section")
    me = lax.axis_index("mp")
    position = ring_position(me, n)
    right, left = ring_member(position + 1, n), ring_member(position - 1, n)
    following, previous = lax.rem(section + 1, sections), lax.rem(section + sections - 1, sections)
    hops = n // 2
    per = n // chunks
    rows, width = x_all.shape[2:]
    length = n * rows
    chunk_rows = per * rows
    qw, kw, vw = wq.shape[0], wk.shape[0], wv.shape[0]
    heads = qw // HD
    group_size = heads * n // KV_HEADS
    nn = (((1,), (0,)), ((), ()))
    nt = (((1,), (1,)), ((), ()))

    stage = pltpu.make_async_copy(arriving, staged, stage_sem)
    stage.start()
    gain_copy = pltpu.make_async_copy(gain_hbm, gain, gain_sem)
    gain_copy.start()
    tables_copy = pltpu.make_async_copy(tables_hbm, tables, tables_sem)
    tables_copy.start()
    barrier = pltpu.get_barrier_semaphore()
    for step in range(1, n):
        pl.semaphore_signal(barrier, inc=1, device_id={"mp": lax.rem(me + step, n)}, device_id_type=MESH)
    for partner in (following, previous):
        pl.semaphore_signal(barrier, inc=1, device_id={"section": partner}, device_id_type=MESH)

    def weight_copy(j, part):
        src, start, size = ((wq, 0, qw), (wk, qw, kw), (wv, qw + kw, vw))[part]
        return pltpu.make_async_copy(
            src.at[:, pl.ds(j * width, width)], weights.at[j, pl.ds(start, size)], w_sem.at[j, part]
        )

    def shift_copy(c):
        return pltpu.make_async_remote_copy(
            src_ref=staged.at[pl.ds(c * per, per)],
            dst_ref=x_all.at[me, pl.ds(c * per, per)],
            send_sem=shift_send.at[c], recv_sem=shift_recv.at[c],
            device_id={"section": following}, device_id_type=MESH,
        )

    def ring_copy(way, hop, c):
        origin = ring_member(position - (hop - 1) if way == 0 else position + (hop - 1), n)
        return pltpu.make_async_remote_copy(
            src_ref=x_all.at[origin, pl.ds(c * per, per)],
            dst_ref=x_all.at[origin, pl.ds(c * per, per)],
            send_sem=ring_send.at[way, hop - 1, c], recv_sem=ring_recv.at[way, hop - 1, c],
            device_id={"mp": right if way == 0 else left}, device_id_type=MESH,
        )

    for j in range(n):
        for part in range(3):
            weight_copy(j, part).start()
    stage.wait()
    pl.semaphore_wait(barrier, n + 1)
    for c in range(chunks):
        shift_copy(c).start()
    acc[...] = jnp.zeros_like(acc)
    squares[...] = jnp.zeros_like(squares)

    def compute(slot, c):
        x = x_all[slot, pl.ds(c * per, per)].astype(jnp.float32).reshape(chunk_rows, width)
        total = x[:, :128] * x[:, :128]
        for g in range(1, width // 128):
            part = x[:, g * 128 : (g + 1) * 128]
            total = total + part * part
        squares[c] += total
        scaled = (x * gain[slot].astype(jnp.float32)).astype(jnp.bfloat16)
        acc[c] += lax.dot_general(scaled, weights[slot], nt, preferred_element_type=jnp.float32)

    for c in range(chunks):
        shift_copy(c).wait_recv()
        ring_copy(0, 1, c).start()
        ring_copy(1, 1, c).start()
    for j in range(n):
        for part in range(3):
            weight_copy(j, part).wait()
    gain_copy.wait()
    tables_copy.wait()
    wo_copy = pltpu.make_async_copy(w_hbm, w_out, wo_sem)
    wo_copy.start()

    @pl.loop(0, chunks)
    def _(c):
        compute(me, c)

    cos, sin = tables[0], tables[1]
    lane = lax.broadcasted_iota(jnp.int32, (HD, kw), 1)
    source = lax.broadcasted_iota(jnp.int32, (HD, kw), 0)
    pick = (source == (me * kw + lane) // (2 * KV_HEADS) * 2 + lane % 2).astype(jnp.float32)
    k_cos = lax.dot_general(cos, pick, nn, precision=lax.Precision.HIGHEST, preferred_element_type=jnp.float32)
    k_sin = lax.dot_general(sin, pick, nn, precision=lax.Precision.HIGHEST, preferred_element_type=jnp.float32)
    per_head = kw // KV_HEADS
    target = lax.broadcasted_iota(jnp.int32, (kw, kw), 0)
    origin_row = lax.broadcasted_iota(jnp.int32, (kw, kw), 1)
    head, within = target // per_head, target % per_head
    order = (origin_row == (within // 2 * KV_HEADS + head) * 2 + within % 2).astype(jnp.bfloat16)

    @pl.loop(0, hops * chunks)
    def _(i):
        hop = i // chunks + 1
        turn = lax.rem(i, chunks)
        last = hop == hops
        c = jnp.where(last, turn // 2 + lax.rem(turn, 2) * (chunks // 2), turn)
        low = c < chunks // 2
        for way in range(2):
            mine = low if way == 0 else jnp.logical_not(low)

            @pl.when(jnp.logical_or(jnp.logical_not(last), mine))
            def _():
                ring_copy(way, hop, c).wait_recv()

            @pl.when(jnp.logical_and(hop < hops, jnp.logical_or(hop + 1 < hops, mine)))
            def _():
                ring_copy(way, hop + 1, c).start()

        @pl.loop(0, 2)
        def _(way):
            mine = low == (way == 0)

            @pl.when(jnp.logical_or(jnp.logical_not(last), mine))
            def _():
                compute(ring_member(jnp.where(way == 0, position - hop, position + hop), n), c)

    inverse = lax.rsqrt(
        jnp.sum(squares[...].reshape(length, 128), axis=1, keepdims=True) * (1.0 / (n * width)) + NORM_EPS
    )
    k = acc[:, :, qw : qw + kw].reshape(length, kw) * inverse
    k_rot = (k * k_cos + swap_pairs(k) * k_sin).astype(jnp.bfloat16)
    def kv_copy(part, step):
        other = lax.rem(me + step, n)
        return pltpu.make_async_remote_copy(
            src_ref=sent.at[other * heads // group_size, part], dst_ref=got.at[me, part],
            send_sem=kv_send.at[part, step - 1], recv_sem=kv_recv.at[part, step - 1],
            device_id={"mp": other}, device_id_type=MESH,
        )

    def order_and_send(part, channels):
        ordered = lax.dot_general(order, channels, nt, preferred_element_type=jnp.float32)
        for h in range(KV_HEADS):
            sent[h, part] = ordered[h * per_head : (h + 1) * per_head].astype(jnp.bfloat16)
        for step in range(1, n):
            kv_copy(part, step).start()

    order_and_send(0, k_rot)
    order_and_send(1, (acc[:, :, qw + kw :].reshape(length, vw) * inverse).astype(jnp.bfloat16))
    got[me] = sent[me * heads // group_size]
    for h in range(heads):
        q = acc[:, :, h * HD : (h + 1) * HD].reshape(length, HD) * inverse
        q_ref[:, :, h * HD : (h + 1) * HD] = (
            (q * cos + swap_pairs(q) * sin).reshape(n, rows, HD).astype(jnp.bfloat16)
        )

    def receive(part, whole):
        for step in range(1, n):
            kv_copy(part, step).wait_recv()
        for j in range(n):
            heads_kv[part, j * per_head : (j + 1) * per_head] = got[j, part].astype(jnp.float32)
        whole[...] = heads_kv[part].astype(jnp.bfloat16)

    receive(0, key_head)

    piece_width = running.shape[4]
    scale = 1.0 / math.sqrt(HD)

    def attend(block, ready=None):
        row = lax.broadcasted_iota(jnp.int32, (rows, length), 0) + block * rows
        column = lax.broadcasted_iota(jnp.int32, (rows, length), 1)
        probs = []
        for h in range(heads):
            q = q_ref[block, :, h * HD : (h + 1) * HD]
            scores = lax.dot_general(q, key_head[...], nn, preferred_element_type=jnp.float32) * scale
            scores = jnp.where(row >= column, scores, -1e30)
            exponent = jnp.exp(scores - jnp.max(scores, axis=1, keepdims=True))
            probs.append((exponent / jnp.sum(exponent, axis=1, keepdims=True)).astype(jnp.bfloat16))
        if ready is not None:
            ready()
        for h in range(heads):
            context[block, :, h * HD : (h + 1) * HD] = lax.dot_general(
                probs[h], value_head[...], nt, preferred_element_type=jnp.float32
            ).astype(jnp.bfloat16)

    def block_of(way, step):
        return ring_member(position - 1 - step if way == 0 else position + 1 + step, n)

    def term(way, step, piece):
        start = (way * pieces + piece) * piece_width
        return jnp.dot(
            context[block_of(way, step)], w_out[:, start : start + piece_width], preferred_element_type=jnp.float32
        )

    def sum_copy(way, step, piece):
        return pltpu.make_async_remote_copy(
            src_ref=running.at[way, step, piece],
            dst_ref=running.at[way, step + 1, piece],
            send_sem=send_sem.at[way, step, piece], recv_sem=recv_sem.at[way, step, piece],
            device_id={"mp": right if way == 0 else left}, device_id_type=MESH,
        )

    wo_copy.wait()
    for way in range(2):
        attend(block_of(way, 0), functools.partial(receive, 1, value_head) if way == 0 else None)
        for piece in range(pieces):
            running[way, 0, piece] = term(way, 0, piece).astype(jnp.bfloat16)
            sum_copy(way, 0, piece).start()

    def ahead(step):
        @pl.when(step < n // 2)
        def _():
            attend(block_of(0, step))
            attend(block_of(1, step))

        @pl.when(step == n // 2)
        def _():
            attend(me)

    ahead(1)

    @pl.loop(1, n - 1)
    def _(step):
        for piece in range(pieces):
            for way in range(2):
                value = term(way, step, piece)
                sum_copy(way, step - 1, piece).wait_recv()
                running[way, step, piece] = (running[way, step, piece].astype(jnp.float32) + value).astype(jnp.bfloat16)
                sum_copy(way, step, piece).start()
        ahead(step + 1)

    for j in range(n):
        stream_ref[:, j * width : (j + 1) * width] = x_all[j, me]
    for piece in range(pieces):
        for way in range(2):
            value = term(way, n - 1, piece)
            sum_copy(way, n - 2, piece).wait_recv()
            value = running[way, n - 1, piece].astype(jnp.float32) + value
            columns = slice((way * pieces + piece) * piece_width, (way * pieces + piece + 1) * piece_width)
            attended_ref[:, columns] = value.astype(jnp.bfloat16)
            stream_ref[:, columns] = (stream_ref[:, columns].astype(jnp.float32) + value).astype(jnp.bfloat16)

    for c in range(chunks):
        shift_copy(c).wait_send()
    for part in range(2):
        for step in range(1, n):
            kv_copy(part, step).wait_send()

    @pl.loop(0, hops * chunks)
    def _(i):
        hop = i // chunks + 1
        c = lax.rem(i, chunks)
        for way in range(2):
            mine = (c < chunks // 2) if way == 0 else (c >= chunks // 2)

            @pl.when(jnp.logical_or(hop < hops, mine))
            def _():
                ring_copy(way, hop, c).wait_send()

    @pl.loop(0, n - 1)
    def _(step):
        for piece in range(pieces):
            for way in range(2):
                sum_copy(way, step, piece).wait_send()


def grid_kernel(
    n, chunks, pieces, arriving, gain_hbm, wq, wk, wv, w_hbm, tables_hbm,
    attended_ref, stream_ref,
    staged, gain, tables, x_all, weights, acc, squares, rotary, sent, got, key_head, value_head, q_ref,
    context, w_half, leaving, entering, summed, final,
    stage_sem, gain_sem, tables_sem, w_sem, shift_send, shift_recv, ring_send, ring_recv, short_send, kv_send, kv_recv,
    wo_own, wo_send, wo_recv, context_send, context_recv, mid_send, mid_recv, final_send, final_recv,
):
    sections = lax.axis_size("section")
    section = lax.axis_index("section")
    me = lax.axis_index("mp")
    position = ring_position(me, n)
    right, left = ring_member(position + 1, n), ring_member(position - 1, n)
    following, previous = lax.rem(section + 1, sections), lax.rem(section + sections - 1, sections)
    hops = n // 2
    rows = attended_ref.shape[0]
    length, width = x_all.shape[1:]
    per = length // chunks
    qw, kw, vw = wq.shape[0], wk.shape[0], wv.shape[0]
    heads = qw // HD
    group_size = heads * n // KV_HEADS
    nn = (((1,), (0,)), ((), ()))
    nt = (((1,), (1,)), ((), ()))

    def part_of(c):
        return pl.ds(pl.multiple_of(c * per, per), per)

    z, x = me // 2, lax.rem(me, 2)
    half = z // 2
    inner_row = 1 + half
    inner = z == inner_row
    corner = jnp.logical_not(inner)
    out_way = lax.rem(position, 2)
    partner = 2 * z + 1 - x
    opposite = 2 * (2 - half) + x
    beyond = ring_member(jnp.where(out_way == 1, position + 1, position - 1), n)
    slot = jnp.where(inner, 2, 0) + x
    per_half = n // 2
    half_first = half * per_half

    stage = pltpu.make_async_copy(arriving, staged, stage_sem)
    stage.start()
    gain_copy = pltpu.make_async_copy(gain_hbm, gain, gain_sem)
    gain_copy.start()
    tables_copy = pltpu.make_async_copy(tables_hbm, tables, tables_sem)
    tables_copy.start()
    barrier = pltpu.get_barrier_semaphore()
    for step in range(1, n):
        pl.semaphore_signal(barrier, inc=1, device_id={"mp": lax.rem(me + step, n)}, device_id_type=MESH)
    for partner_section in (following, previous):
        pl.semaphore_signal(barrier, inc=1, device_id={"section": partner_section}, device_id_type=MESH)

    def weight_copy(j, part):
        src, start, size = ((wq, 0, qw), (wk, qw, kw), (wv, qw + kw, vw))[part]
        return pltpu.make_async_copy(
            src.at[:, pl.ds(j * width, width)], weights.at[j, pl.ds(start, size)], w_sem.at[j, part]
        )

    def shift_copy(c):
        return pltpu.make_async_remote_copy(
            src_ref=staged.at[part_of(c)],
            dst_ref=x_all.at[me, part_of(c)],
            send_sem=shift_send.at[c], recv_sem=shift_recv.at[c],
            device_id={"section": following}, device_id_type=MESH,
        )

    def share_of(way, c):
        return pl.ds(pl.multiple_of(c * per + way * (per // 2), per // 2), per // 2)

    def ring_copy(way, hop, c, shared):
        origin = ring_member(position - (hop - 1) if way == 0 else position + (hop - 1), n)
        tokens = share_of(way, c) if shared else part_of(c)
        return pltpu.make_async_remote_copy(
            src_ref=x_all.at[origin, tokens], dst_ref=x_all.at[origin, tokens],
            send_sem=ring_send.at[way, hop - 1, c], recv_sem=ring_recv.at[way, hop - 1, c],
            device_id={"mp": right if way == 0 else left}, device_id_type=MESH,
        )

    def short_copy(late, c):
        origin = beyond if late else me
        tokens = share_of(out_way, c) if late else part_of(c)
        return pltpu.make_async_remote_copy(
            src_ref=x_all.at[origin, tokens], dst_ref=x_all.at[origin, tokens],
            send_sem=short_send.at[late, c], recv_sem=ring_recv.at[out_way, hops - 2 + late, c],
            device_id={"mp": partner}, device_id_type=MESH,
        )

    def through(way):
        return jnp.logical_or(inner, out_way != way)

    piece_width = w_half.shape[3]

    def wo_source(target, k):
        owner = jnp.where(target == 0, x, 1 - x)
        start = pl.multiple_of(owner * (pieces * piece_width) + k * piece_width, piece_width)
        return w_hbm.at[:, pl.ds(start, piece_width)], 2 * inner_row + owner

    def wo_copy(target, k):
        src, device = wo_source(target, k)
        return pltpu.make_async_remote_copy(
            src_ref=src, dst_ref=w_half.at[k, slot],
            send_sem=wo_send.at[target, k], recv_sem=wo_recv.at[slot, k],
            device_id={"mp": device}, device_id_type=MESH,
        )

    def wo_own_copy(k):
        src, _ = wo_source(0, k)
        return pltpu.make_async_copy(src, w_half.at[k, slot], wo_own.at[k])

    def wo_arrived(s, k):
        return pltpu.make_async_remote_copy(
            src_ref=w_half.at[k, s], dst_ref=w_half.at[k, s],
            send_sem=wo_send.at[0, k], recv_sem=wo_recv.at[s, k],
            device_id={"mp": partner}, device_id_type=MESH,
        )

    for j in range(n):
        for part in range(3):
            weight_copy(j, part).start()
    stage.wait()
    pl.semaphore_wait(barrier, n + 1)
    for c in range(chunks):
        shift_copy(c).start()
    acc[...] = jnp.zeros_like(acc)
    squares[...] = jnp.zeros_like(squares)
    key_head[...] = jnp.zeros_like(key_head)
    value_head[...] = jnp.zeros_like(value_head)

    def compute(source, c):
        block = x_all[source, part_of(c)].astype(jnp.float32)
        total = block[:, :128] * block[:, :128]
        for g in range(1, width // 128):
            part = block[:, g * 128 : (g + 1) * 128]
            total = total + part * part
        squares[c] += total
        scaled = (block * gain[source].astype(jnp.float32)).astype(jnp.bfloat16)
        acc[c] += lax.dot_general(scaled, weights[source], nt, preferred_element_type=jnp.float32)

    def start_own(c):
        shift_copy(c).wait_recv()
        ring_copy(0, 1, c, False).start()
        ring_copy(1, 1, c, False).start()

        @pl.when(inner)
        def _():
            short_copy(0, c).start()

    for c in range(AHEAD):
        start_own(c)
    for j in range(n):
        for part in range(3):
            weight_copy(j, part).wait()
    gain_copy.wait()
    tables_copy.wait()

    @pl.when(inner)
    def _():
        @pl.loop(0, pieces)
        def _(k):
            wo_own_copy(k).start()

    lane = lax.broadcasted_iota(jnp.int32, (HD, kw), 1)
    source = lax.broadcasted_iota(jnp.int32, (HD, kw), 0)
    pick = (source == (me * kw + lane) // (2 * KV_HEADS) * 2 + lane % 2).astype(jnp.float32)
    for t in range(2):
        picked = lax.dot_general(
            tables[t].reshape(length, HD), pick, nn, precision=lax.Precision.HIGHEST, preferred_element_type=jnp.float32
        )
        rotary[t] = picked.reshape(chunks, per, kw)
    per_head = kw // KV_HEADS
    target = lax.broadcasted_iota(jnp.int32, (kw, kw), 0)
    origin_row = lax.broadcasted_iota(jnp.int32, (kw, kw), 1)
    head, within = target // per_head, target % per_head
    order = (origin_row == (within // 2 * KV_HEADS + head) * 2 + within % 2).astype(jnp.bfloat16)

    def kv_copy(c, step):
        other = lax.rem(me + step, n)
        return pltpu.make_async_remote_copy(
            src_ref=sent.at[c, other * heads // group_size], dst_ref=got.at[c, me],
            send_sem=kv_send.at[c, step - 1], recv_sem=kv_recv.at[c, step - 1],
            device_id={"mp": other}, device_id_type=MESH,
        )

    def project(c):
        inverse = lax.rsqrt(jnp.sum(squares[c], axis=1, keepdims=True) * (1.0 / (n * width)) + NORM_EPS)
        k = acc[c, :, qw : qw + kw] * inverse
        k_rot = (k * rotary[0, c] + swap_pairs(k) * rotary[1, c]).astype(jnp.bfloat16)
        v = (acc[c, :, qw + kw :] * inverse).astype(jnp.bfloat16)
        for part, channels in enumerate((k_rot, v)):
            ordered = lax.dot_general(order, channels, nt, preferred_element_type=jnp.float32)
            for h in range(KV_HEADS):
                sent[c, h, part] = ordered[h * per_head : (h + 1) * per_head].astype(jnp.bfloat16)
        for step in range(1, n):
            kv_copy(c, step).start()
        got[c, me] = sent[c, me * heads // group_size]
        for h in range(heads):
            q = acc[c, :, h * HD : (h + 1) * HD] * inverse
            q_ref[c, :, h * HD : (h + 1) * HD] = (q * tables[0, c] + swap_pairs(q) * tables[1, c]).astype(jnp.bfloat16)

    scale = 1.0 / (math.sqrt(HD) * math.log(2.0))

    def attend(c):
        for step in range(1, n):
            kv_copy(c, step).wait_recv()
        for j in range(n):
            key_head[j * per_head : (j + 1) * per_head, part_of(c)] = got[c, j, 0]
            value_head[j * per_head : (j + 1) * per_head, part_of(c)] = got[c, j, 1]
        row = lax.broadcasted_iota(jnp.int32, (per, length), 0) + c * per
        column = lax.broadcasted_iota(jnp.int32, (per, length), 1)
        for h in range(heads):
            q = q_ref[c, :, h * HD : (h + 1) * HD]
            scores = lax.dot_general(q, key_head[...], nn, preferred_element_type=jnp.float32)
            scores = jnp.where(row >= column, scores, -1e30)
            exponent = jnp.exp2((scores - jnp.max(scores, axis=1, keepdims=True)) * scale)
            probs = (exponent * (1.0 / jnp.sum(exponent, axis=1, keepdims=True))).astype(jnp.bfloat16)
            context[slot, part_of(c), h * HD : (h + 1) * HD] = lax.dot_general(
                probs, value_head[...], nt, preferred_element_type=jnp.float32
            ).astype(jnp.bfloat16)

        @pl.when(corner)
        def _():
            context_copy(0, c).start()

        context_copy(1, c).start()

    def context_copy(target, c):
        return pltpu.make_async_remote_copy(
            src_ref=context.at[slot, part_of(c)], dst_ref=context.at[slot, part_of(c)],
            send_sem=context_send.at[target, c], recv_sem=context_recv.at[slot, c],
            device_id={"mp": 2 * inner_row + (x if target == 0 else 1 - x)}, device_id_type=MESH,
        )

    def context_arrived(s, c):
        return pltpu.make_async_remote_copy(
            src_ref=context.at[s, part_of(c)], dst_ref=context.at[s, part_of(c)],
            send_sem=context_send.at[0, c], recv_sem=context_recv.at[s, c],
            device_id={"mp": partner}, device_id_type=MESH,
        )

    slots = context.shape[0]
    parts = per_half
    half_chunks = chunks // 2
    turns = parts * pieces

    def turn_of(i):
        late = i - HEAD * parts
        part = jnp.where(late < 0, i // HEAD, lax.rem(i - HEAD * parts + turns, parts))
        piece = jnp.where(late < 0, lax.rem(i, HEAD), HEAD + late // parts)
        return part, piece

    def term(group, part, k):
        start = pl.multiple_of((group * per_half + part) * rows, rows)
        total = jnp.zeros((rows, piece_width), jnp.float32)
        for s in range(slots):
            total += jnp.dot(
                context[s, pl.ds(start, rows)], w_half[k, s], preferred_element_type=jnp.float32
            )
        return total

    def mid_copy(i):
        return pltpu.make_async_remote_copy(
            src_ref=leaving.at[i], dst_ref=entering.at[i],
            send_sem=mid_send.at[i], recv_sem=mid_recv.at[i],
            device_id={"mp": opposite}, device_id_type=MESH,
        )

    def final_copy(i):
        part, k = turn_of(i)
        return pltpu.make_async_remote_copy(
            src_ref=summed.at[i], dst_ref=final.at[x, k],
            send_sem=final_send.at[i], recv_sem=final_recv.at[x, k],
            device_id={"mp": half_first + part}, device_id_type=MESH,
        )

    def final_arrived(side, k):
        return pltpu.make_async_remote_copy(
            src_ref=final.at[side, k], dst_ref=final.at[side, k],
            send_sem=final_send.at[k], recv_sem=final_recv.at[side, k],
            device_id={"mp": partner}, device_id_type=MESH,
        )

    def contexts_arrived(group, i):
        @pl.when(jnp.logical_and(lax.rem(i, HEAD) == 0, i // HEAD < half_chunks))
        def _():
            for s in range(slots):
                @pl.when(slot != s)
                def _():
                    context_arrived(s, group * half_chunks + i // HEAD).wait_recv()

    def send_turn(i):
        part, k = turn_of(i)

        @pl.when(part == 0)
        def _():
            wo_own_copy(k).wait()
            for s in range(slots):
                @pl.when(slot != s)
                def _():
                    wo_arrived(s, k).wait_recv()
        contexts_arrived(1 - half, i)
        leaving[i] = term(1 - half, part, k).astype(jnp.bfloat16)
        mid_copy(i).start()

    def wo_range(first, last):
        @pl.loop(first, last)
        def _(i):
            wo_copy(lax.rem(i, 2), i // 2).start()

    @pl.loop(0, chunks + hops - 1)
    def _(wave):
        @pl.when(wave + AHEAD < chunks)
        def _():
            start_own(wave + AHEAD)

        @pl.when(wave < chunks)
        def _():
            compute(me, wave)

        @pl.when(jnp.logical_and(inner, wave == chunks + hops - 2))
        def _():
            @pl.loop(0, FIRST)
            def _(i):
                send_turn(i)

        @pl.when(jnp.logical_and(wave > hops, wave < chunks + hops - 2))
        def _():
            attend(wave - hops - 1)

        @pl.loop(1, hops + 1)
        def _(hop):
            c = wave - (hop - 1)
            last = hop == hops

            @pl.when(jnp.logical_and(c >= 0, c < chunks))
            def _():
                for way in range(2):
                    @pl.when(jnp.logical_not(last))
                    def _():
                        ring_copy(way, hop, c, False).wait_recv()

                    @pl.when(last)
                    def _():
                        ring_copy(way, hop, c, True).wait_recv()

                    @pl.when(jnp.logical_or(hop < hops - 2, jnp.logical_and(hop == hops - 2, through(way))))
                    def _():
                        ring_copy(way, hop + 1, c, False).start()

                    @pl.when(jnp.logical_and(hop == hops - 1, through(way)))
                    def _():
                        ring_copy(way, hop + 1, c, True).start()

                    @pl.when(jnp.logical_and(jnp.logical_and(inner, out_way == way), hop == 1))
                    def _():
                        short_copy(1, c).start()

                @pl.when(jnp.logical_and(inner, hop == SLOT_INNER))
                def _():
                    @pl.loop(c * EARLY_INNER // chunks, (c + 1) * EARLY_INNER // chunks)
                    def _(k):
                        wo_copy(1, k).start()

                @pl.when(jnp.logical_and(corner, hop == SLOT_CORNER))
                def _():
                    wo_range(c * EARLY_CORNER // chunks, (c + 1) * EARLY_CORNER // chunks)

                @pl.when(jnp.logical_and(c == chunks - 1, hop == hops - 1))
                def _():
                    attend(chunks - 3)

                    @pl.when(corner)
                    def _():
                        wo_range(EARLY_CORNER, EARLY_CORNER + MORE)

                @pl.loop(0, jnp.where(last, 1, 2))
                def _(way):
                    compute(ring_member(jnp.where(way == 0, position - hop, position + hop), n), c)

        @pl.when(wave >= hops - 1)
        def _():
            project(wave - (hops - 1))

    @pl.loop(START, turns + LEAD)
    def _(i):
        @pl.when(jnp.logical_or(i == LAST - 1, i == LAST))
        def _():
            attend(chunks - 2 + i - (LAST - 1))

        @pl.when(jnp.logical_and(corner, i == LAST))
        def _():
            wo_range(EARLY_CORNER + MORE, 2 * pieces)

        @pl.when(inner)
        def _():
            @pl.when(i == LAST)
            def _():
                @pl.loop(EARLY_INNER, pieces)
                def _(k):
                    wo_copy(1, k).start()

            @pl.when(jnp.logical_and(i >= FIRST, i < turns))
            def _():
                send_turn(i)

            @pl.when(i >= LEAD)
            def _():
                j = i - LEAD
                part, k = turn_of(j)
                contexts_arrived(half, j)
                value = term(half, part, k)
                mid_copy(j).wait_recv()
                value = value + entering[j].astype(jnp.float32)
                value = value.astype(jnp.bfloat16)

                @pl.when(half_first + part != me)
                def _():
                    summed[j] = value
                    final_copy(j).start()

                @pl.when(half_first + part == me)
                def _():
                    final[x, k] = value

    @pl.loop(0, pieces)
    def _(k):
        for side in range(2):
            @pl.when(jnp.logical_or(corner, x != side))
            def _():
                final_arrived(side, k).wait_recv()
            start = side * (pieces * piece_width) + k * piece_width
            columns = pl.ds(pl.multiple_of(start, piece_width), piece_width)
            within_block = pl.ds(pl.multiple_of(lax.rem(start, width), piece_width), piece_width)
            value = final[side, k]
            attended_ref[:, columns] = value
            stream_ref[:, columns] = (
                x_all[start // width, pl.ds(pl.multiple_of(me * rows, rows), rows), within_block].astype(jnp.float32) + value.astype(jnp.float32)
            ).astype(jnp.bfloat16)

    for c in range(chunks):
        shift_copy(c).wait_send()

    @pl.loop(0, chunks)
    def _(c):
        for step in range(1, n):
            kv_copy(c, step).wait_send()

        @pl.when(corner)
        def _():
            context_copy(0, c).wait_send()
        context_copy(1, c).wait_send()

    @pl.loop(0, chunks)
    def _(c):
        for way in range(2):
            @pl.loop(1, hops - 1)
            def _(hop):
                ring_copy(way, hop, c, False).wait_send()

            @pl.when(through(way))
            def _():
                ring_copy(way, hops - 1, c, False).wait_send()
                ring_copy(way, hops, c, True).wait_send()

    @pl.loop(0, pieces)
    def _(k):
        wo_copy(1, k).wait_send()

        @pl.when(corner)
        def _():
            wo_copy(0, k).wait_send()

    @pl.when(inner)
    def _():
        @pl.loop(0, turns)
        def _(i):
            part, k = turn_of(i)
            mid_copy(i).wait_send()

            @pl.when(half_first + part != me)
            def _():
                final_copy(i).wait_send()

    @pl.when(inner)
    def _():
        for c in range(chunks):
            short_copy(0, c).wait_send()
            short_copy(1, c).wait_send()


def rotary_tables(length):
    pair = (np.arange(HD) // 2).astype(np.float32)
    frequency = np.exp(pair * np.float32(-2.0 * math.log(ROPE_BASE) / HD)).astype(np.float32)
    angles = frequency[None, :] * np.arange(length, dtype=np.float32)[:, None]
    sign = np.where(np.arange(HD) % 2 == 0, -1.0, 1.0).astype(np.float32)
    return np.stack([np.cos(angles), np.sin(angles) * sign]).astype(np.float32)


def local(arriving, norm_gain, w_query, w_key, w_value, w_out):
    n = lax.axis_size("mp")
    length, width = arriving.shape[1:]
    rows = length // n
    full = n * width
    chunks = 8 if n <= 8 else 2
    pieces = 4 if n <= 8 else 2
    qw, kw, vw = w_query.shape[1], w_key.shape[1], w_value.shape[1]
    tables = rotary_tables(length)
    vmem = pl.BlockSpec(memory_space=pltpu.VMEM)
    hbm = pl.BlockSpec(memory_space=pltpu.HBM)
    bf16, f32 = jnp.bfloat16, jnp.float32
    dma = pltpu.SemaphoreType.DMA
    if n == 8:
        pieces = 8
        piece_width = full // (2 * pieces)
        per = 128
        chunks = length // per
        per_head = kw // KV_HEADS
        turns = n // 2 * pieces
        kernel = grid_kernel
        operands = (
            arriving[0],
            norm_gain[0].reshape(n, 1, width),
            w_query[0], w_key[0], w_value[0], w_out[0], jnp.asarray(tables.reshape(2, chunks, per, HD)),
        )
        scratch = [
            pltpu.VMEM((length, width), bf16),
            pltpu.VMEM((n, 1, width), bf16),
            pltpu.VMEM((2, chunks, per, HD), f32),
            pltpu.VMEM((n, length, width), bf16),
            pltpu.VMEM((n, qw + kw + vw, width), bf16),
            pltpu.VMEM((chunks, per, qw + kw + vw), f32),
            pltpu.VMEM((chunks, per, 128), f32),
            pltpu.VMEM((2, chunks, per, kw), f32),
            pltpu.VMEM((chunks, KV_HEADS, 2, per_head, per), bf16),
            pltpu.VMEM((chunks, n, 2, per_head, per), bf16),
            pltpu.VMEM((HD, length), bf16),
            pltpu.VMEM((HD, length), bf16),
            pltpu.VMEM((chunks, per, qw), bf16),
            pltpu.VMEM((4, length, qw), bf16),
            pltpu.VMEM((pieces, 4, qw, piece_width), bf16),
            pltpu.VMEM((turns, rows, piece_width), bf16),
            pltpu.VMEM((turns, rows, piece_width), bf16),
            pltpu.VMEM((turns, rows, piece_width), bf16),
            pltpu.VMEM((2, pieces, rows, piece_width), bf16),
            dma(()),
            dma(()),
            dma(()),
            dma((n, 3)),
            dma((chunks,)),
            dma((chunks,)),
            dma((2, n // 2, chunks)),
            dma((2, n // 2, chunks)),
            dma((2, chunks)),
            dma((chunks, n - 1)),
            dma((chunks, n - 1)),
            dma((pieces,)),
            dma((2, pieces)),
            dma((4, pieces)),
            dma((2, chunks)),
            dma((4, chunks)),
            dma((turns,)),
            dma((turns,)),
            dma((turns,)),
            dma((2, pieces)),
        ]
    else:
        kernel = ring_kernel
        operands = (
            arriving[0].reshape(n, rows, width),
            norm_gain[0].reshape(n, 1, width),
            w_query[0], w_key[0], w_value[0], w_out[0], jnp.asarray(tables),
        )
        scratch = [
            pltpu.VMEM((n, rows, width), bf16),
            pltpu.VMEM((n, 1, width), bf16),
            pltpu.VMEM((2, length, HD), f32),
            pltpu.VMEM((n, n, rows, width), bf16),
            pltpu.VMEM((n, qw + kw + vw, width), bf16),
            pltpu.VMEM((chunks, length // chunks, qw + kw + vw), f32),
            pltpu.VMEM((chunks, length // chunks, 128), f32),
            pltpu.VMEM((KV_HEADS, 2, kw // KV_HEADS, length), bf16),
            pltpu.VMEM((n, 2, kw // KV_HEADS, length), bf16),
            pltpu.VMEM((2, HD, length), f32),
            pltpu.VMEM((HD, length), bf16),
            pltpu.VMEM((HD, length), bf16),
            pltpu.VMEM((n, rows, qw), bf16),
            pltpu.VMEM((qw, full), bf16),
            pltpu.VMEM((n, rows, qw), bf16),
            pltpu.VMEM((2, n, pieces, rows, full // (2 * pieces)), bf16),
            dma(()),
            dma(()),
            dma(()),
            dma((n, 3)),
            dma(()),
            dma((chunks,)),
            dma((chunks,)),
            dma((2, n // 2, chunks)),
            dma((2, n // 2, chunks)),
            dma((2, n - 1)),
            dma((2, n - 1)),
            dma((2, n - 1, pieces)),
            dma((2, n - 1, pieces)),
        ]
    attended, stream = pl.pallas_call(
        functools.partial(kernel, n, chunks, pieces),
        name="layer",
        out_shape=(pltpu.VMEM((rows, full), bf16),) * 2,
        in_specs=[hbm] * 7,
        out_specs=(vmem, vmem),
        scratch_shapes=scratch,
        compiler_params=pltpu.CompilerParams(collective_id=0, has_side_effects=True, vmem_limit_bytes=VMEM_LIMIT),
    )(*operands)
    return (attended[None], stream[None])


def solution(mesh):
    return jax.shard_map(
        local,
        mesh=mesh,
        in_specs=(
            P("section", None, "mp"),
            P("section", None),
            P("section", "mp", None),
            P("section", "mp", None),
            P("section", "mp", None),
            P("section", "mp", None),
        ),
        out_specs=(P("section", "mp", None), P("section", "mp", None)),
        check_vma=False,
    )
```

```python
import functools
import math

import jax
import jax.numpy as jnp
import numpy as np
from jax import lax
from jax.experimental import pallas as pl
from jax.experimental.pallas import tpu as pltpu
from jax.sharding import PartitionSpec as P

HD = 128
KV_HEADS = 8
ROPE_BASE = 500000.0
NORM_EPS = 1e-05
MESH = pl.DeviceIdType.MESH
VMEM_LIMIT = 63500000
AHEAD = 2
LEAD = 4
FIRST = 2
START = 1
LAST = 3
SLOT_CORNER = 2
SLOT_INNER = 2
EARLY_CORNER = 7
EARLY_INNER = 5
MORE = 0
HEAD = 3


def ring_position(member, n):
    return jnp.where(member % 2 == 0, member // 2, n - 1 - member // 2)


def ring_member(position, n):
    position = lax.rem(position + 2 * n, n)
    return jnp.where(position < n // 2, 2 * position, 2 * (n - 1 - position) + 1)


def swap_pairs(x):
    lane = lax.broadcasted_iota(jnp.int32, x.shape, 1)
    width = x.shape[1]
    return jnp.where(lane % 2 == 0, pltpu.roll(x, width - 1, 1), pltpu.roll(x, 1, 1))


def ring_kernel(
    n, chunks, pieces, arriving, gain_hbm, wq, wk, wv, w_hbm, tables_hbm,
    attended_ref, stream_ref,
    staged, gain, tables, x_all, weights, acc, squares, sent, got, heads_kv, key_head, value_head, q_ref, w_out, context, running,
    stage_sem, gain_sem, tables_sem, w_sem, wo_sem, shift_send, shift_recv, ring_send, ring_recv, kv_send, kv_recv, send_sem, recv_sem,
):
    sections = lax.axis_size("section")
    section = lax.axis_index("section")
    me = lax.axis_index("mp")
    position = ring_position(me, n)
    right, left = ring_member(position + 1, n), ring_member(position - 1, n)
    following, previous = lax.rem(section + 1, sections), lax.rem(section + sections - 1, sections)
    hops = n // 2
    per = n // chunks
    rows, width = x_all.shape[2:]
    length = n * rows
    chunk_rows = per * rows
    qw, kw, vw = wq.shape[0], wk.shape[0], wv.shape[0]
    heads = qw // HD
    group_size = heads * n // KV_HEADS
    nn = (((1,), (0,)), ((), ()))
    nt = (((1,), (1,)), ((), ()))

    stage = pltpu.make_async_copy(arriving, staged, stage_sem)
    stage.start()
    gain_copy = pltpu.make_async_copy(gain_hbm, gain, gain_sem)
    gain_copy.start()
    tables_copy = pltpu.make_async_copy(tables_hbm, tables, tables_sem)
    tables_copy.start()
    barrier = pltpu.get_barrier_semaphore()
    for step in range(1, n):
        pl.semaphore_signal(barrier, inc=1, device_id={"mp": lax.rem(me + step, n)}, device_id_type=MESH)
    for partner in (following, previous):
        pl.semaphore_signal(barrier, inc=1, device_id={"section": partner}, device_id_type=MESH)

    def weight_copy(j, part):
        src, start, size = ((wq, 0, qw), (wk, qw, kw), (wv, qw + kw, vw))[part]
        return pltpu.make_async_copy(
            src.at[:, pl.ds(j * width, width)], weights.at[j, pl.ds(start, size)], w_sem.at[j, part]
        )

    def shift_copy(c):
        return pltpu.make_async_remote_copy(
            src_ref=staged.at[pl.ds(c * per, per)],
            dst_ref=x_all.at[me, pl.ds(c * per, per)],
            send_sem=shift_send.at[c], recv_sem=shift_recv.at[c],
            device_id={"section": following}, device_id_type=MESH,
        )

    def ring_copy(way, hop, c):
        origin = ring_member(position - (hop - 1) if way == 0 else position + (hop - 1), n)
        return pltpu.make_async_remote_copy(
            src_ref=x_all.at[origin, pl.ds(c * per, per)],
            dst_ref=x_all.at[origin, pl.ds(c * per, per)],
            send_sem=ring_send.at[way, hop - 1, c], recv_sem=ring_recv.at[way, hop - 1, c],
            device_id={"mp": right if way == 0 else left}, device_id_type=MESH,
        )

    for j in range(n):
        for part in range(3):
            weight_copy(j, part).start()
    stage.wait()
    pl.semaphore_wait(barrier, n + 1)
    for c in range(chunks):
        shift_copy(c).start()
    acc[...] = jnp.zeros_like(acc)
    squares[...] = jnp.zeros_like(squares)

    def compute(slot, c):
        x = x_all[slot, pl.ds(c * per, per)].astype(jnp.float32).reshape(chunk_rows, width)
        total = x[:, :128] * x[:, :128]
        for g in range(1, width // 128):
            part = x[:, g * 128 : (g + 1) * 128]
            total = total + part * part
        squares[c] += total
        scaled = (x * gain[slot].astype(jnp.float32)).astype(jnp.bfloat16)
        acc[c] += lax.dot_general(scaled, weights[slot], nt, preferred_element_type=jnp.float32)

    for c in range(chunks):
        shift_copy(c).wait_recv()
        ring_copy(0, 1, c).start()
        ring_copy(1, 1, c).start()
    for j in range(n):
        for part in range(3):
            weight_copy(j, part).wait()
    gain_copy.wait()
    tables_copy.wait()
    wo_copy = pltpu.make_async_copy(w_hbm, w_out, wo_sem)
    wo_copy.start()

    @pl.loop(0, chunks)
    def _(c):
        compute(me, c)

    cos, sin = tables[0], tables[1]
    lane = lax.broadcasted_iota(jnp.int32, (HD, kw), 1)
    source = lax.broadcasted_iota(jnp.int32, (HD, kw), 0)
    pick = (source == (me * kw + lane) // (2 * KV_HEADS) * 2 + lane % 2).astype(jnp.float32)
    k_cos = lax.dot_general(cos, pick, nn, precision=lax.Precision.HIGHEST, preferred_element_type=jnp.float32)
    k_sin = lax.dot_general(sin, pick, nn, precision=lax.Precision.HIGHEST, preferred_element_type=jnp.float32)
    per_head = kw // KV_HEADS
    target = lax.broadcasted_iota(jnp.int32, (kw, kw), 0)
    origin_row = lax.broadcasted_iota(jnp.int32, (kw, kw), 1)
    head, within = target // per_head, target % per_head
    order = (origin_row == (within // 2 * KV_HEADS + head) * 2 + within % 2).astype(jnp.bfloat16)

    @pl.loop(0, hops * chunks)
    def _(i):
        hop = i // chunks + 1
        turn = lax.rem(i, chunks)
        last = hop == hops
        c = jnp.where(last, turn // 2 + lax.rem(turn, 2) * (chunks // 2), turn)
        low = c < chunks // 2
        for way in range(2):
            mine = low if way == 0 else jnp.logical_not(low)

            @pl.when(jnp.logical_or(jnp.logical_not(last), mine))
            def _():
                ring_copy(way, hop, c).wait_recv()

            @pl.when(jnp.logical_and(hop < hops, jnp.logical_or(hop + 1 < hops, mine)))
            def _():
                ring_copy(way, hop + 1, c).start()

        @pl.loop(0, 2)
        def _(way):
            mine = low == (way == 0)

            @pl.when(jnp.logical_or(jnp.logical_not(last), mine))
            def _():
                compute(ring_member(jnp.where(way == 0, position - hop, position + hop), n), c)

    inverse = lax.rsqrt(
        jnp.sum(squares[...].reshape(length, 128), axis=1, keepdims=True) * (1.0 / (n * width)) + NORM_EPS
    )
    k = acc[:, :, qw : qw + kw].reshape(length, kw) * inverse
    k_rot = (k * k_cos + swap_pairs(k) * k_sin).astype(jnp.bfloat16)
    def kv_copy(part, step):
        other = lax.rem(me + step, n)
        return pltpu.make_async_remote_copy(
            src_ref=sent.at[other * heads // group_size, part], dst_ref=got.at[me, part],
            send_sem=kv_send.at[part, step - 1], recv_sem=kv_recv.at[part, step - 1],
            device_id={"mp": other}, device_id_type=MESH,
        )

    def order_and_send(part, channels):
        ordered = lax.dot_general(order, channels, nt, preferred_element_type=jnp.float32)
        for h in range(KV_HEADS):
            sent[h, part] = ordered[h * per_head : (h + 1) * per_head].astype(jnp.bfloat16)
        for step in range(1, n):
            kv_copy(part, step).start()

    order_and_send(0, k_rot)
    order_and_send(1, (acc[:, :, qw + kw :].reshape(length, vw) * inverse).astype(jnp.bfloat16))
    got[me] = sent[me * heads // group_size]
    for h in range(heads):
        q = acc[:, :, h * HD : (h + 1) * HD].reshape(length, HD) * inverse
        q_ref[:, :, h * HD : (h + 1) * HD] = (
            (q * cos + swap_pairs(q) * sin).reshape(n, rows, HD).astype(jnp.bfloat16)
        )

    def receive(part, whole):
        for step in range(1, n):
            kv_copy(part, step).wait_recv()
        for j in range(n):
            heads_kv[part, j * per_head : (j + 1) * per_head] = got[j, part].astype(jnp.float32)
        whole[...] = heads_kv[part].astype(jnp.bfloat16)

    receive(0, key_head)

    piece_width = running.shape[4]
    scale = 1.0 / math.sqrt(HD)

    def attend(block, ready=None):
        row = lax.broadcasted_iota(jnp.int32, (rows, length), 0) + block * rows
        column = lax.broadcasted_iota(jnp.int32, (rows, length), 1)
        probs = []
        for h in range(heads):
            q = q_ref[block, :, h * HD : (h + 1) * HD]
            scores = lax.dot_general(q, key_head[...], nn, preferred_element_type=jnp.float32) * scale
            scores = jnp.where(row >= column, scores, -1e30)
            exponent = jnp.exp(scores - jnp.max(scores, axis=1, keepdims=True))
            probs.append((exponent / jnp.sum(exponent, axis=1, keepdims=True)).astype(jnp.bfloat16))
        if ready is not None:
            ready()
        for h in range(heads):
            context[block, :, h * HD : (h + 1) * HD] = lax.dot_general(
                probs[h], value_head[...], nt, preferred_element_type=jnp.float32
            ).astype(jnp.bfloat16)

    def block_of(way, step):
        return ring_member(position - 1 - step if way == 0 else position + 1 + step, n)

    def term(way, step, piece):
        start = (way * pieces + piece) * piece_width
        return jnp.dot(
            context[block_of(way, step)], w_out[:, start : start + piece_width], preferred_element_type=jnp.float32
        )

    def sum_copy(way, step, piece):
        return pltpu.make_async_remote_copy(
            src_ref=running.at[way, step, piece],
            dst_ref=running.at[way, step + 1, piece],
            send_sem=send_sem.at[way, step, piece], recv_sem=recv_sem.at[way, step, piece],
            device_id={"mp": right if way == 0 else left}, device_id_type=MESH,
        )

    wo_copy.wait()
    for way in range(2):
        attend(block_of(way, 0), functools.partial(receive, 1, value_head) if way == 0 else None)
        for piece in range(pieces):
            running[way, 0, piece] = term(way, 0, piece).astype(jnp.bfloat16)
            sum_copy(way, 0, piece).start()

    def ahead(step):
        @pl.when(step < n // 2)
        def _():
            attend(block_of(0, step))
            attend(block_of(1, step))

        @pl.when(step == n // 2)
        def _():
            attend(me)

    ahead(1)

    @pl.loop(1, n - 1)
    def _(step):
        for piece in range(pieces):
            for way in range(2):
                value = term(way, step, piece)
                sum_copy(way, step - 1, piece).wait_recv()
                running[way, step, piece] = (running[way, step, piece].astype(jnp.float32) + value).astype(jnp.bfloat16)
                sum_copy(way, step, piece).start()
        ahead(step + 1)

    for j in range(n):
        stream_ref[:, j * width : (j + 1) * width] = x_all[j, me]
    for piece in range(pieces):
        for way in range(2):
            value = term(way, n - 1, piece)
            sum_copy(way, n - 2, piece).wait_recv()
            value = running[way, n - 1, piece].astype(jnp.float32) + value
            columns = slice((way * pieces + piece) * piece_width, (way * pieces + piece + 1) * piece_width)
            attended_ref[:, columns] = value.astype(jnp.bfloat16)
            stream_ref[:, columns] = (stream_ref[:, columns].astype(jnp.float32) + value).astype(jnp.bfloat16)

    for c in range(chunks):
        shift_copy(c).wait_send()
    for part in range(2):
        for step in range(1, n):
            kv_copy(part, step).wait_send()

    @pl.loop(0, hops * chunks)
    def _(i):
        hop = i // chunks + 1
        c = lax.rem(i, chunks)
        for way in range(2):
            mine = (c < chunks // 2) if way == 0 else (c >= chunks // 2)

            @pl.when(jnp.logical_or(hop < hops, mine))
            def _():
                ring_copy(way, hop, c).wait_send()

    @pl.loop(0, n - 1)
    def _(step):
        for piece in range(pieces):
            for way in range(2):
                sum_copy(way, step, piece).wait_send()


def grid_kernel(
    n, chunks, pieces, arriving, gain_hbm, wq, wk, wv, w_hbm, tables_hbm,
    attended_ref, stream_ref,
    staged, gain, tables, x_all, weights, acc, squares, rotary, sent, got, key_head, value_head, q_ref,
    context, w_half, leaving, entering, summed, final,
    stage_sem, gain_sem, tables_sem, w_sem, shift_send, shift_recv, ring_send, ring_recv, short_send, kv_send, kv_recv,
    wo_own, wo_send, wo_recv, context_send, context_recv, mid_send, mid_recv, final_send, final_recv,
):
    sections = lax.axis_size("section")
    section = lax.axis_index("section")
    me = lax.axis_index("mp")
    position = ring_position(me, n)
    right, left = ring_member(position + 1, n), ring_member(position - 1, n)
    following, previous = lax.rem(section + 1, sections), lax.rem(section + sections - 1, sections)
    hops = n // 2
    rows = attended_ref.shape[0]
    length, width = x_all.shape[1:]
    per = length // chunks
    qw, kw, vw = wq.shape[0], wk.shape[0], wv.shape[0]
    heads = qw // HD
    group_size = heads * n // KV_HEADS
    nn = (((1,), (0,)), ((), ()))
    nt = (((1,), (1,)), ((), ()))

    def part_of(c):
        return pl.ds(pl.multiple_of(c * per, per), per)

    z, x = me // 2, lax.rem(me, 2)
    half = z // 2
    inner_row = 1 + half
    inner = z == inner_row
    corner = jnp.logical_not(inner)
    out_way = lax.rem(position, 2)
    partner = 2 * z + 1 - x
    opposite = 2 * (2 - half) + x
    beyond = ring_member(jnp.where(out_way == 1, position + 1, position - 1), n)
    slot = jnp.where(inner, 2, 0) + x
    per_half = n // 2
    half_first = half * per_half

    stage = pltpu.make_async_copy(arriving, staged, stage_sem)
    stage.start()
    gain_copy = pltpu.make_async_copy(gain_hbm, gain, gain_sem)
    gain_copy.start()
    tables_copy = pltpu.make_async_copy(tables_hbm, tables, tables_sem)
    tables_copy.start()
    barrier = pltpu.get_barrier_semaphore()
    for step in range(1, n):
        pl.semaphore_signal(barrier, inc=1, device_id={"mp": lax.rem(me + step, n)}, device_id_type=MESH)
    for partner_section in (following, previous):
        pl.semaphore_signal(barrier, inc=1, device_id={"section": partner_section}, device_id_type=MESH)

    def weight_copy(j, part):
        src, start, size = ((wq, 0, qw), (wk, qw, kw), (wv, qw + kw, vw))[part]
        return pltpu.make_async_copy(
            src.at[:, pl.ds(j * width, width)], weights.at[j, pl.ds(start, size)], w_sem.at[j, part]
        )

    def shift_copy(c):
        return pltpu.make_async_remote_copy(
            src_ref=staged.at[part_of(c)],
            dst_ref=x_all.at[me, part_of(c)],
            send_sem=shift_send.at[c], recv_sem=shift_recv.at[c],
            device_id={"section": following}, device_id_type=MESH,
        )

    def share_of(way, c):
        return pl.ds(pl.multiple_of(c * per + way * (per // 2), per // 2), per // 2)

    def ring_copy(way, hop, c, shared):
        origin = ring_member(position - (hop - 1) if way == 0 else position + (hop - 1), n)
        tokens = share_of(way, c) if shared else part_of(c)
        return pltpu.make_async_remote_copy(
            src_ref=x_all.at[origin, tokens], dst_ref=x_all.at[origin, tokens],
            send_sem=ring_send.at[way, hop - 1, c], recv_sem=ring_recv.at[way, hop - 1, c],
            device_id={"mp": right if way == 0 else left}, device_id_type=MESH,
        )

    def short_copy(late, c):
        origin = beyond if late else me
        tokens = share_of(out_way, c) if late else part_of(c)
        return pltpu.make_async_remote_copy(
            src_ref=x_all.at[origin, tokens], dst_ref=x_all.at[origin, tokens],
            send_sem=short_send.at[late, c], recv_sem=ring_recv.at[out_way, hops - 2 + late, c],
            device_id={"mp": partner}, device_id_type=MESH,
        )

    def through(way):
        return jnp.logical_or(inner, out_way != way)

    piece_width = w_half.shape[3]

    def wo_source(target, k):
        owner = jnp.where(target == 0, x, 1 - x)
        start = pl.multiple_of(owner * (pieces * piece_width) + k * piece_width, piece_width)
        return w_hbm.at[:, pl.ds(start, piece_width)], 2 * inner_row + owner

    def wo_copy(target, k):
        src, device = wo_source(target, k)
        return pltpu.make_async_remote_copy(
            src_ref=src, dst_ref=w_half.at[k, slot],
            send_sem=wo_send.at[target, k], recv_sem=wo_recv.at[slot, k],
            device_id={"mp": device}, device_id_type=MESH,
        )

    def wo_own_copy(k):
        src, _ = wo_source(0, k)
        return pltpu.make_async_copy(src, w_half.at[k, slot], wo_own.at[k])

    def wo_arrived(s, k):
        return pltpu.make_async_remote_copy(
            src_ref=w_half.at[k, s], dst_ref=w_half.at[k, s],
            send_sem=wo_send.at[0, k], recv_sem=wo_recv.at[s, k],
            device_id={"mp": partner}, device_id_type=MESH,
        )

    for j in range(n):
        for part in range(3):
            weight_copy(j, part).start()
    stage.wait()
    pl.semaphore_wait(barrier, n + 1)
    for c in range(chunks):
        shift_copy(c).start()
    acc[...] = jnp.zeros_like(acc)
    squares[...] = jnp.zeros_like(squares)
    key_head[...] = jnp.zeros_like(key_head)
    value_head[...] = jnp.zeros_like(value_head)

    def compute(source, c):
        block = x_all[source, part_of(c)].astype(jnp.float32)
        total = block[:, :128] * block[:, :128]
        for g in range(1, width // 128):
            part = block[:, g * 128 : (g + 1) * 128]
            total = total + part * part
        squares[c] += total
        scaled = (block * gain[source].astype(jnp.float32)).astype(jnp.bfloat16)
        acc[c] += lax.dot_general(scaled, weights[source], nt, preferred_element_type=jnp.float32)

    def start_own(c):
        shift_copy(c).wait_recv()
        ring_copy(0, 1, c, False).start()
        ring_copy(1, 1, c, False).start()

        @pl.when(inner)
        def _():
            short_copy(0, c).start()

    for c in range(AHEAD):
        start_own(c)
    for j in range(n):
        for part in range(3):
            weight_copy(j, part).wait()
    gain_copy.wait()
    tables_copy.wait()

    @pl.when(inner)
    def _():
        @pl.loop(0, pieces)
        def _(k):
            wo_own_copy(k).start()

    lane = lax.broadcasted_iota(jnp.int32, (HD, kw), 1)
    source = lax.broadcasted_iota(jnp.int32, (HD, kw), 0)
    pick = (source == (me * kw + lane) // (2 * KV_HEADS) * 2 + lane % 2).astype(jnp.float32)
    for t in range(2):
        picked = lax.dot_general(
            tables[t].reshape(length, HD), pick, nn, precision=lax.Precision.HIGHEST, preferred_element_type=jnp.float32
        )
        rotary[t] = picked.reshape(chunks, per, kw)
    per_head = kw // KV_HEADS
    target = lax.broadcasted_iota(jnp.int32, (kw, kw), 0)
    origin_row = lax.broadcasted_iota(jnp.int32, (kw, kw), 1)
    head, within = target // per_head, target % per_head
    order = (origin_row == (within // 2 * KV_HEADS + head) * 2 + within % 2).astype(jnp.bfloat16)

    def kv_copy(c, step):
        other = lax.rem(me + step, n)
        return pltpu.make_async_remote_copy(
            src_ref=sent.at[c, other * heads // group_size], dst_ref=got.at[c, me],
            send_sem=kv_send.at[c, step - 1], recv_sem=kv_recv.at[c, step - 1],
            device_id={"mp": other}, device_id_type=MESH,
        )

    def project(c):
        inverse = lax.rsqrt(jnp.sum(squares[c], axis=1, keepdims=True) * (1.0 / (n * width)) + NORM_EPS)
        k = acc[c, :, qw : qw + kw] * inverse
        k_rot = (k * rotary[0, c] + swap_pairs(k) * rotary[1, c]).astype(jnp.bfloat16)
        v = (acc[c, :, qw + kw :] * inverse).astype(jnp.bfloat16)
        for part, channels in enumerate((k_rot, v)):
            ordered = lax.dot_general(order, channels, nt, preferred_element_type=jnp.float32)
            for h in range(KV_HEADS):
                sent[c, h, part] = ordered[h * per_head : (h + 1) * per_head].astype(jnp.bfloat16)
        for step in range(1, n):
            kv_copy(c, step).start()
        got[c, me] = sent[c, me * heads // group_size]
        for h in range(heads):
            q = acc[c, :, h * HD : (h + 1) * HD] * inverse
            q_ref[c, :, h * HD : (h + 1) * HD] = (q * tables[0, c] + swap_pairs(q) * tables[1, c]).astype(jnp.bfloat16)

    scale = 1.0 / (math.sqrt(HD) * math.log(2.0))

    def attend(c):
        for step in range(1, n):
            kv_copy(c, step).wait_recv()
        for j in range(n):
            key_head[j * per_head : (j + 1) * per_head, part_of(c)] = got[c, j, 0]
            value_head[j * per_head : (j + 1) * per_head, part_of(c)] = got[c, j, 1]
        row = lax.broadcasted_iota(jnp.int32, (per, length), 0) + c * per
        column = lax.broadcasted_iota(jnp.int32, (per, length), 1)
        for h in range(heads):
            q = q_ref[c, :, h * HD : (h + 1) * HD]
            scores = lax.dot_general(q, key_head[...], nn, preferred_element_type=jnp.float32)
            scores = jnp.where(row >= column, scores, -1e30)
            exponent = jnp.exp2((scores - jnp.max(scores, axis=1, keepdims=True)) * scale)
            probs = (exponent * (1.0 / jnp.sum(exponent, axis=1, keepdims=True))).astype(jnp.bfloat16)
            context[slot, part_of(c), h * HD : (h + 1) * HD] = lax.dot_general(
                probs, value_head[...], nt, preferred_element_type=jnp.float32
            ).astype(jnp.bfloat16)

        @pl.when(corner)
        def _():
            context_copy(0, c).start()

        context_copy(1, c).start()

    def context_copy(target, c):
        return pltpu.make_async_remote_copy(
            src_ref=context.at[slot, part_of(c)], dst_ref=context.at[slot, part_of(c)],
            send_sem=context_send.at[target, c], recv_sem=context_recv.at[slot, c],
            device_id={"mp": 2 * inner_row + (x if target == 0 else 1 - x)}, device_id_type=MESH,
        )

    def context_arrived(s, c):
        return pltpu.make_async_remote_copy(
            src_ref=context.at[s, part_of(c)], dst_ref=context.at[s, part_of(c)],
            send_sem=context_send.at[0, c], recv_sem=context_recv.at[s, c],
            device_id={"mp": partner}, device_id_type=MESH,
        )

    slots = context.shape[0]
    parts = per_half
    half_chunks = chunks // 2
    turns = parts * pieces

    def turn_of(i):
        late = i - HEAD * parts
        part = jnp.where(late < 0, i // HEAD, lax.rem(i - HEAD * parts + turns, parts))
        piece = jnp.where(late < 0, lax.rem(i, HEAD), HEAD + late // parts)
        return part, piece

    def term(group, part, k):
        start = pl.multiple_of((group * per_half + part) * rows, rows)
        total = jnp.zeros((rows, piece_width), jnp.float32)
        for s in range(slots):
            total += jnp.dot(
                context[s, pl.ds(start, rows)], w_half[k, s], preferred_element_type=jnp.float32
            )
        return total

    def mid_copy(i):
        return pltpu.make_async_remote_copy(
            src_ref=leaving.at[i], dst_ref=entering.at[i],
            send_sem=mid_send.at[i], recv_sem=mid_recv.at[i],
            device_id={"mp": opposite}, device_id_type=MESH,
        )

    def final_copy(i):
        part, k = turn_of(i)
        return pltpu.make_async_remote_copy(
            src_ref=summed.at[i], dst_ref=final.at[x, k],
            send_sem=final_send.at[i], recv_sem=final_recv.at[x, k],
            device_id={"mp": half_first + part}, device_id_type=MESH,
        )

    def final_arrived(side, k):
        return pltpu.make_async_remote_copy(
            src_ref=final.at[side, k], dst_ref=final.at[side, k],
            send_sem=final_send.at[k], recv_sem=final_recv.at[side, k],
            device_id={"mp": partner}, device_id_type=MESH,
        )

    def contexts_arrived(group, i):
        @pl.when(jnp.logical_and(lax.rem(i, HEAD) == 0, i // HEAD < half_chunks))
        def _():
            for s in range(slots):
                @pl.when(slot != s)
                def _():
                    context_arrived(s, group * half_chunks + i // HEAD).wait_recv()

    def send_turn(i):
        part, k = turn_of(i)

        @pl.when(part == 0)
        def _():
            wo_own_copy(k).wait()
            for s in range(slots):
                @pl.when(slot != s)
                def _():
                    wo_arrived(s, k).wait_recv()
        contexts_arrived(1 - half, i)
        leaving[i] = term(1 - half, part, k).astype(jnp.bfloat16)
        mid_copy(i).start()

    def wo_range(first, last):
        @pl.loop(first, last)
        def _(i):
            wo_copy(lax.rem(i, 2), i // 2).start()

    @pl.loop(0, chunks + hops - 1)
    def _(wave):
        @pl.when(wave + AHEAD < chunks)
        def _():
            start_own(wave + AHEAD)

        @pl.when(wave < chunks)
        def _():
            compute(me, wave)

        @pl.when(jnp.logical_and(inner, wave == chunks + hops - 2))
        def _():
            @pl.loop(0, FIRST)
            def _(i):
                send_turn(i)

        @pl.when(jnp.logical_and(wave > hops, wave < chunks + hops - 2))
        def _():
            attend(wave - hops - 1)

        @pl.loop(1, hops + 1)
        def _(hop):
            c = wave - (hop - 1)
            last = hop == hops

            @pl.when(jnp.logical_and(c >= 0, c < chunks))
            def _():
                for way in range(2):
                    @pl.when(jnp.logical_not(last))
                    def _():
                        ring_copy(way, hop, c, False).wait_recv()

                    @pl.when(last)
                    def _():
                        ring_copy(way, hop, c, True).wait_recv()

                    @pl.when(jnp.logical_or(hop < hops - 2, jnp.logical_and(hop == hops - 2, through(way))))
                    def _():
                        ring_copy(way, hop + 1, c, False).start()

                    @pl.when(jnp.logical_and(hop == hops - 1, through(way)))
                    def _():
                        ring_copy(way, hop + 1, c, True).start()

                    @pl.when(jnp.logical_and(jnp.logical_and(inner, out_way == way), hop == 1))
                    def _():
                        short_copy(1, c).start()

                @pl.when(jnp.logical_and(inner, hop == SLOT_INNER))
                def _():
                    @pl.loop(c * EARLY_INNER // chunks, (c + 1) * EARLY_INNER // chunks)
                    def _(k):
                        wo_copy(1, k).start()

                @pl.when(jnp.logical_and(corner, hop == SLOT_CORNER))
                def _():
                    wo_range(c * EARLY_CORNER // chunks, (c + 1) * EARLY_CORNER // chunks)

                @pl.when(jnp.logical_and(c == chunks - 1, hop == hops - 1))
                def _():
                    attend(chunks - 3)

                    @pl.when(corner)
                    def _():
                        wo_range(EARLY_CORNER, EARLY_CORNER + MORE)

                @pl.loop(0, jnp.where(last, 1, 2))
                def _(way):
                    compute(ring_member(jnp.where(way == 0, position - hop, position + hop), n), c)

        @pl.when(wave >= hops - 1)
        def _():
            project(wave - (hops - 1))

    @pl.loop(START, turns + LEAD)
    def _(i):
        @pl.when(jnp.logical_or(i == LAST - 1, i == LAST))
        def _():
            attend(chunks - 2 + i - (LAST - 1))

        @pl.when(jnp.logical_and(corner, i == LAST))
        def _():
            wo_range(EARLY_CORNER + MORE, 2 * pieces)

        @pl.when(inner)
        def _():
            @pl.when(i == LAST)
            def _():
                @pl.loop(EARLY_INNER, pieces)
                def _(k):
                    wo_copy(1, k).start()

            @pl.when(jnp.logical_and(i >= FIRST, i < turns))
            def _():
                send_turn(i)

            @pl.when(i >= LEAD)
            def _():
                j = i - LEAD
                part, k = turn_of(j)
                contexts_arrived(half, j)
                value = term(half, part, k)
                mid_copy(j).wait_recv()
                value = value + entering[j].astype(jnp.float32)
                value = value.astype(jnp.bfloat16)

                @pl.when(half_first + part != me)
                def _():
                    summed[j] = value
                    final_copy(j).start()

                @pl.when(half_first + part == me)
                def _():
                    final[x, k] = value

    @pl.loop(0, pieces)
    def _(k):
        for side in range(2):
            @pl.when(jnp.logical_or(corner, x != side))
            def _():
                final_arrived(side, k).wait_recv()
            start = side * (pieces * piece_width) + k * piece_width
            columns = pl.ds(pl.multiple_of(start, piece_width), piece_width)
            within_block = pl.ds(pl.multiple_of(lax.rem(start, width), piece_width), piece_width)
            value = final[side, k]
            attended_ref[:, columns] = value
            stream_ref[:, columns] = (
                x_all[start // width, pl.ds(pl.multiple_of(me * rows, rows), rows), within_block].astype(jnp.float32) + value.astype(jnp.float32)
            ).astype(jnp.bfloat16)

    for c in range(chunks):
        shift_copy(c).wait_send()

    @pl.loop(0, chunks)
    def _(c):
        for step in range(1, n):
            kv_copy(c, step).wait_send()

        @pl.when(corner)
        def _():
            context_copy(0, c).wait_send()
        context_copy(1, c).wait_send()

    @pl.loop(0, chunks)
    def _(c):
        for way in range(2):
            @pl.loop(1, hops - 1)
            def _(hop):
                ring_copy(way, hop, c, False).wait_send()

            @pl.when(through(way))
            def _():
                ring_copy(way, hops - 1, c, False).wait_send()
                ring_copy(way, hops, c, True).wait_send()

    @pl.loop(0, pieces)
    def _(k):
        wo_copy(1, k).wait_send()

        @pl.when(corner)
        def _():
            wo_copy(0, k).wait_send()

    @pl.when(inner)
    def _():
        @pl.loop(0, turns)
        def _(i):
            part, k = turn_of(i)
            mid_copy(i).wait_send()

            @pl.when(half_first + part != me)
            def _():
                final_copy(i).wait_send()

    @pl.when(inner)
    def _():
        for c in range(chunks):
            short_copy(0, c).wait_send()
            short_copy(1, c).wait_send()


def rotary_tables(length):
    pair = (np.arange(HD) // 2).astype(np.float32)
    frequency = np.exp(pair * np.float32(-2.0 * math.log(ROPE_BASE) / HD)).astype(np.float32)
    angles = frequency[None, :] * np.arange(length, dtype=np.float32)[:, None]
    sign = np.where(np.arange(HD) % 2 == 0, -1.0, 1.0).astype(np.float32)
    return np.stack([np.cos(angles), np.sin(angles) * sign]).astype(np.float32)


def local(arriving, norm_gain, w_query, w_key, w_value, w_out):
    n = lax.axis_size("mp")
    length, width = arriving.shape[1:]
    rows = length // n
    full = n * width
    chunks = 8 if n <= 8 else 2
    pieces = 4 if n <= 8 else 2
    qw, kw, vw = w_query.shape[1], w_key.shape[1], w_value.shape[1]
    tables = rotary_tables(length)
    vmem = pl.BlockSpec(memory_space=pltpu.VMEM)
    hbm = pl.BlockSpec(memory_space=pltpu.HBM)
    bf16, f32 = jnp.bfloat16, jnp.float32
    dma = pltpu.SemaphoreType.DMA
    if n == 8:
        pieces = 8
        piece_width = full // (2 * pieces)
        per = 128
        chunks = length // per
        per_head = kw // KV_HEADS
        turns = n // 2 * pieces
        kernel = grid_kernel
        operands = (
            arriving[0],
            norm_gain[0].reshape(n, 1, width),
            w_query[0], w_key[0], w_value[0], w_out[0], jnp.asarray(tables.reshape(2, chunks, per, HD)),
        )
        scratch = [
            pltpu.VMEM((length, width), bf16),
            pltpu.VMEM((n, 1, width), bf16),
            pltpu.VMEM((2, chunks, per, HD), f32),
            pltpu.VMEM((n, length, width), bf16),
            pltpu.VMEM((n, qw + kw + vw, width), bf16),
            pltpu.VMEM((chunks, per, qw + kw + vw), f32),
            pltpu.VMEM((chunks, per, 128), f32),
            pltpu.VMEM((2, chunks, per, kw), f32),
            pltpu.VMEM((chunks, KV_HEADS, 2, per_head, per), bf16),
            pltpu.VMEM((chunks, n, 2, per_head, per), bf16),
            pltpu.VMEM((HD, length), bf16),
            pltpu.VMEM((HD, length), bf16),
            pltpu.VMEM((chunks, per, qw), bf16),
            pltpu.VMEM((4, length, qw), bf16),
            pltpu.VMEM((pieces, 4, qw, piece_width), bf16),
            pltpu.VMEM((turns, rows, piece_width), bf16),
            pltpu.VMEM((turns, rows, piece_width), bf16),
            pltpu.VMEM((turns, rows, piece_width), bf16),
            pltpu.VMEM((2, pieces, rows, piece_width), bf16),
            dma(()),
            dma(()),
            dma(()),
            dma((n, 3)),
            dma((chunks,)),
            dma((chunks,)),
            dma((2, n // 2, chunks)),
            dma((2, n // 2, chunks)),
            dma((2, chunks)),
            dma((chunks, n - 1)),
            dma((chunks, n - 1)),
            dma((pieces,)),
            dma((2, pieces)),
            dma((4, pieces)),
            dma((2, chunks)),
            dma((4, chunks)),
            dma((turns,)),
            dma((turns,)),
            dma((turns,)),
            dma((2, pieces)),
        ]
    else:
        kernel = ring_kernel
        operands = (
            arriving[0].reshape(n, rows, width),
            norm_gain[0].reshape(n, 1, width),
            w_query[0], w_key[0], w_value[0], w_out[0], jnp.asarray(tables),
        )
        scratch = [
            pltpu.VMEM((n, rows, width), bf16),
            pltpu.VMEM((n, 1, width), bf16),
            pltpu.VMEM((2, length, HD), f32),
            pltpu.VMEM((n, n, rows, width), bf16),
            pltpu.VMEM((n, qw + kw + vw, width), bf16),
            pltpu.VMEM((chunks, length // chunks, qw + kw + vw), f32),
            pltpu.VMEM((chunks, length // chunks, 128), f32),
            pltpu.VMEM((KV_HEADS, 2, kw // KV_HEADS, length), bf16),
            pltpu.VMEM((n, 2, kw // KV_HEADS, length), bf16),
            pltpu.VMEM((2, HD, length), f32),
            pltpu.VMEM((HD, length), bf16),
            pltpu.VMEM((HD, length), bf16),
            pltpu.VMEM((n, rows, qw), bf16),
            pltpu.VMEM((qw, full), bf16),
            pltpu.VMEM((n, rows, qw), bf16),
            pltpu.VMEM((2, n, pieces, rows, full // (2 * pieces)), bf16),
            dma(()),
            dma(()),
            dma(()),
            dma((n, 3)),
            dma(()),
            dma((chunks,)),
            dma((chunks,)),
            dma((2, n // 2, chunks)),
            dma((2, n // 2, chunks)),
            dma((2, n - 1)),
            dma((2, n - 1)),
            dma((2, n - 1, pieces)),
            dma((2, n - 1, pieces)),
        ]
    attended, stream = pl.pallas_call(
        functools.partial(kernel, n, chunks, pieces),
        name="layer",
        out_shape=(pltpu.VMEM((rows, full), bf16),) * 2,
        in_specs=[hbm] * 7,
        out_specs=(vmem, vmem),
        scratch_shapes=scratch,
        compiler_params=pltpu.CompilerParams(collective_id=0, has_side_effects=True, vmem_limit_bytes=VMEM_LIMIT),
    )(*operands)
    return (attended[None], stream[None])


def solution(mesh):
    return jax.shard_map(
        local,
        mesh=mesh,
        in_specs=(
            P("section", None, "mp"),
            P("section", None),
            P("section", "mp", None),
            P("section", "mp", None),
            P("section", "mp", None),
            P("section", "mp", None),
        ),
        out_specs=(P("section", "mp", None), P("section", "mp", None)),
        check_vma=False,
    )
```
